128 devices in a mesh: lat: 16 (over z_lo, y, core), lon: 8 (over z_hi, x).
Axes of the slice: x: 4, y: 4, z: 4 (z_hi: 2, z_lo: 2; z = z_hi * 2 + z_lo), core: 2. Of those that a mesh axis runs over, the one named last changes fastest.
Arguments:
- tokens: bfloat16 [4, 128, 256, 1024], P(None, 'lat', 'lon'), may hold values from -6 to 6
- qkv_weight: bfloat16 [3072, 1024], P(('lat', 'lon')), may hold values from -0.1875 to 0.1875
- proj_weight: bfloat16 [1024, 1024], P(('lat', 'lon')), may hold values from -0.1875 to 0.1875
- up_weight: bfloat16 [4096, 1024], P(('lat', 'lon')), may hold values from -0.1875 to 0.1875
- down_weight: bfloat16 [4096, 1024], P(('lat', 'lon')), may hold values from -0.09375 to 0.09375
- bias_table: float32 [225, 16], replicated, may hold values from -3 to 220, as said below
- sea_mask: int32 [128, 256], replicated, may hold values 0 or 1
Outputs:
- block_out: bfloat16 [4, 128, 256, 1024], P(None, 'lat', 'lon')
The draws below stay inside these ranges and needn't reach their ends.
Inputs may be any that keep to these rules, and one draw needn't show every extreme that they name: `bias_table`: entry [o, h] is the bias of head h for the in-window offset numbered o as in the reference program.
All inputs are finite; a program needn't handle non-finite values.
Results may differ from the reference program's by a relative error of at most 0.012.
Values may be sent and summed in bfloat16 or wider, within the bound.
A program may use at most 128 MiB of HBM per device.

```python
import jax
import jax.numpy as jnp
from jax import lax

D = 1024
HEADS = 16
MLP = 4096
BATCH = 4
RELPOS = 225
HEAD_DIM = 64
NLAT = 128
NLON = 256


def draw_bias_table(key, part):
    base_key, head_key = jax.random.split(jax.random.fold_in(key, 7))
    bias_rows = jnp.clip(jax.random.normal(base_key, (RELPOS, HEADS), jnp.float32), -3.0, 3.0)
    return bias_rows


def plant(values, stream_key, smallest, top_value):
    place = [jax.random.randint(jax.random.fold_in(stream_key, axis), (), 0, length) for axis, length in enumerate(values.shape)]
    main_axis = values.shape.index(max(values.shape))
    next_to = place[:main_axis] + [(place[main_axis] + 1) % values.shape[main_axis]] + place[main_axis + 1:]
    return values.at[tuple(place)].set(smallest).at[tuple(next_to)].set(top_value)


def shard_levels(rng, shape, pieces, least, top_value):
    level = 1.0
    for position, blocks in pieces:
        steps = jax.random.uniform(jax.random.fold_in(jax.random.fold_in(rng, 6), position), (blocks,), jnp.float32, least / len(pieces), top_value / len(pieces))
        level = level * jnp.repeat(jnp.exp(steps), shape[position] // blocks).reshape((-1,) + (1,) * (len(shape) - 1 - position))
    return level


def noise(rng, dims, deviation, reach, pieces=(), kind=jnp.bfloat16):
    drawn = jax.random.normal(rng, dims, jnp.float32) * deviation
    if len(pieces) > 0:
        drawn = shard_levels(rng, dims, pieces, -0.22, 0.18) * drawn
    return jnp.clip(drawn, min=-reach, max=reach).astype(kind)


def setup_inputs(seed: int = 0) -> dict:
    splits = jax.random.split(jax.random.key(seed), 8)
    return {
        "tokens": noise(splits[0], (BATCH, NLAT, NLON, D), 1.0, 6.0, ((1, 16), (2, 8))),
        "qkv_weight": noise(splits[1], (3 * D, D), D ** -0.5, 0.1875, ((0, 128),)),
        "proj_weight": noise(splits[2], (D, D), D ** -0.5, 0.1875, ((0, 128),)),
        "up_weight": noise(splits[3], (MLP, D), D ** -0.5, 0.1875, ((0, 128),)),
        "down_weight": noise(splits[4], (MLP, D), MLP ** -0.5, 0.09375, ((0, 128),)),
        "bias_table": draw_bias_table(jax.random.fold_in(splits[7], 71), 0),
        "sea_mask": plant((jax.random.randint(splits[6], (NLAT, NLON), 0, 4) < 3).astype(jnp.int32), jax.random.fold_in(splits[6], 1), 0, 1),
    }


def layer_norm(values):
    widened = values.astype(jnp.float32)
    centre = lax.optimization_barrier(jnp.mean(widened, axis=-1, keepdims=True))
    spread = lax.optimization_barrier(jnp.mean(jnp.square(widened - centre), axis=-1, keepdims=True))
    return ((widened - centre) * lax.rsqrt(spread + 1e-05)).astype(jnp.bfloat16)

def offsets_table():
    cell_ids = jnp.arange(64, dtype=jnp.int32)
    row_of = cell_ids // 8
    col_of = cell_ids % 8
    return (row_of[:, None] - row_of[None, :] + 7) * 15 + (col_of[:, None] - col_of[None, :] + 7)

def row_region(row_ids, total_rows):
    return jnp.where(row_ids < 4, 2, jnp.where(row_ids >= total_rows - 4, 1, 0)).astype(jnp.int32)

def reference(tokens, qkv_weight, proj_weight, up_weight, down_weight, bias_table, sea_mask):
    normed = layer_norm(tokens)
    rolled = jnp.roll(normed, (-4, -4), axis=(1, 2))
    sea_rolled = jnp.roll(sea_mask, (-4, -4), axis=(0, 1))
    pos_bias = jnp.transpose(bias_table[offsets_table()], (2, 0, 1))
    same_cell = jnp.eye(64, dtype=bool)
    windows_across = NLON // 8
    row_blocks = jnp.transpose(rolled.reshape(BATCH, NLAT // 8, 8, NLON, D), (1, 0, 2, 3, 4))
    sea_blocks = sea_rolled.reshape(NLAT // 8, 8, NLON)
    score_scale = HEAD_DIM ** (-0.5)

    def window_row(inputs):
        row_block, sea_rows, block_index = inputs
        projected = jnp.dot(row_block.reshape(-1, D), qkv_weight.T, preferred_element_type=jnp.float32).astype(jnp.bfloat16)
        windows = projected.reshape(BATCH, 8, windows_across, 8, 3 * D).transpose(0, 2, 1, 3, 4)
        windows = windows.reshape(BATCH, windows_across, 64, 3, HEADS, HEAD_DIM).astype(jnp.float32)
        queries = windows[:, :, :, 0]
        keys_here = windows[:, :, :, 1]
        values_here = windows[:, :, :, 2]
        scores = jnp.einsum('bsqhd,bskhd->bshqk', queries, keys_here) * score_scale + pos_bias[None, None]
        grid_rows = (block_index * 8 + 4 + jnp.arange(8, dtype=jnp.int32)) % NLAT
        region = jnp.repeat(row_region(grid_rows, NLAT), 8)
        sea_keep = sea_rows.reshape(8, windows_across, 8).transpose(1, 0, 2).reshape(windows_across, 64) == 1
        allowed = (region[:, None] == region[None, :])[None] & (sea_keep[:, None, :] | same_cell[None])
        scores = jnp.where(allowed[None, :, None], scores, -1e+30)
        row_top = lax.optimization_barrier(jnp.max(scores, axis=-1, keepdims=True))
        weights = jnp.exp(scores - row_top)
        attn_probs = (weights / lax.optimization_barrier(jnp.sum(weights, axis=-1, keepdims=True))).astype(jnp.bfloat16)
        context = jnp.einsum('bshqk,bskhd->bsqhd', attn_probs.astype(jnp.float32), values_here).astype(jnp.bfloat16)
        context = context.reshape(BATCH, windows_across, 8, 8, D).transpose(0, 2, 1, 3, 4)
        return context.reshape(BATCH, 8, NLON, D)
    contexts = lax.map(window_row, (row_blocks, sea_blocks, jnp.arange(NLAT // 8, dtype=jnp.int32)))
    context_grid = jnp.transpose(contexts, (1, 0, 2, 3, 4)).reshape(BATCH, NLAT, NLON, D)
    context_grid = jnp.roll(context_grid, (4, 4), axis=(1, 2))

    def finish(inputs):
        token_block, context_block = inputs
        attention_out = jnp.dot(context_block.reshape(-1, D), proj_weight.T, preferred_element_type=jnp.float32)
        attended = (token_block.reshape(-1, D).astype(jnp.float32) + attention_out).astype(jnp.bfloat16)
        normed_two = layer_norm(attended)
        hidden = jax.nn.gelu(jnp.dot(normed_two, up_weight.T, preferred_element_type=jnp.float32)).astype(jnp.bfloat16)
        result = attended.astype(jnp.float32) + jnp.dot(hidden, down_weight, preferred_element_type=jnp.float32)
        return result.astype(jnp.bfloat16).reshape(token_block.shape)
    token_rows = jnp.transpose(tokens.reshape(BATCH, NLAT // 8, 8, NLON, D), (1, 0, 2, 3, 4))
    context_rows = jnp.transpose(context_grid.reshape(BATCH, NLAT // 8, 8, NLON, D), (1, 0, 2, 3, 4))
    finished = lax.map(finish, (token_rows, context_rows))
    return jnp.transpose(finished, (1, 0, 2, 3, 4)).reshape(BATCH, NLAT, NLON, D)
```

```python
import jax
import jax.numpy as jnp
from jax import lax
from jax.experimental import pallas as pl
from jax.experimental.pallas import tpu as pltpu
from jax.sharding import PartitionSpec as P

MESH = pl.DeviceIdType.MESH
BF = jnp.bfloat16
F32 = jnp.float32
D = 1024
BLK = 512
FAR = -1e30

PIECES = {
    "qa": (0, 0, 8, "xyz"),
    "qb": (0, 8, 8, "yzx"),
    "qc": (0, 16, 8, "zxy"),
    "ua": (2, 0, 16, "xyz"),
    "ub": (2, 16, 8, "yzx"),
    "pc": (1, 0, 8, "zxy"),
    "uc": (2, 24, 8, "zxy"),
    "da": (3, 0, 8, "xyz"),
    "db": (3, 8, 16, "yzx"),
    "dc": (3, 24, 8, "zxy"),
}
NAMES = list(PIECES)
PER = 15

FIRST = ["qa", "qb", "qc"]
LATER = ["pc", "ua", "ub", "uc", "da", "db", "dc"]
PLAN = [
    ("start", [(2, n) for n in FIRST] + [(3, n) for n in FIRST] + [(4, n) for n in FIRST]),
    ("start", [(2, n) for n in LATER[:4]] + [(3, n) for n in LATER[:4]]),
    ("norm", [(5, n) for n in FIRST] + [(4, n) for n in LATER[:4]]),
    ("norm", [(6, n) for n in FIRST] + [(7, n) for n in FIRST]),
    ("qkv1", [(2, n) for n in LATER[4:]]),
    ("qkv2", [(3, n) for n in LATER[4:]]),
    ("qkv3", [(5, "ub"), (5, "pc")]),
    ("att0", [(4, "db"), (6, "ub"), (6, "pc")]),
    ("att3", [(5, "ua")]),
    ("att5", [(5, "uc"), (4, "da"), (4, "dc")]),
    ("att10", [(6, "ua")]),
    ("att12", [(6, "uc"), (7, "pc")]),
    ("proj0", [(5, "da"), (5, "db")]),
    ("proj2", [(5, "dc")]),
    ("up0", [(7, "ua"), (7, "ub"), (7, "uc")]),
    ("up2", [(6, "da")]),
    ("up4", [(6, "dc")]),
    ("up5", [(6, "db")]),
    ("down0", [(7, "da"), (7, "db"), (7, "dc")]),
]


def planned(slot):
    steps = []
    for name, listed in PLAN:
        if name == slot:
            steps += listed
    return steps


def block_kernel(
    tok, wq_in, wp_in, wu_in, wd_in, bias, keys,
    out,
    wq, wp, wu, wd, ext, normed, qkv, att, hid, back, side,
    w_send, w_recv, own_sem, h_send, h_recv, r_send, r_recv, t_sem,
):
    lat = lax.axis_index("lat")
    lon = lax.axis_index("lon")
    core = lat % 2
    y = (lat // 2) % 4
    z_lo = lat // 8
    x = lon % 4
    z_hi = lon // 4
    at = {"x": x, "y": y, "z": z_hi * 2 + z_lo}

    def device(over, partner=False):
        c = dict(at)
        c.update(over)
        k = 1 - core if partner else core
        return {"lat": ((c["z"] % 2) * 4 + c["y"]) * 2 + k, "lon": (c["z"] // 2) * 4 + c["x"]}

    def near(axis, by):
        return (at[axis] + by + 4) % 4

    def shifted(d_lat, d_lon):
        return {"lat": (lat + d_lat + 16) % 16, "lon": (lon + d_lon + 8) % 8}

    held = (wq, wp, wu, wd)
    shards = (wq_in, wp_in, wu_in, wd_in)

    def region(name, c, where):
        which, first, rows, _ = PIECES[name]
        ref = held[which]

        def part(axis):
            v = where[axis]
            if v is None:
                return slice(None)
            if isinstance(v, tuple):
                return pl.ds(2 * v[1], 2)
            return v

        v = where["z"]
        if v is None:
            lo, hi = slice(None), slice(None)
        elif isinstance(v, tuple):
            lo, hi = v[1], slice(None)
        else:
            lo, hi = v % 2, v // 2
        return ref.at[lo, part("y"), c, hi, part("x"), pl.ds(first, rows)]

    def weight_copy(name, slot, where, to, partner=False, src=None):
        k = NAMES.index(name) * PER + slot
        there = region(name, core, where)
        return pltpu.make_async_remote_copy(
            src_ref=there if src is None else src,
            dst_ref=there,
            send_sem=w_send.at[k],
            recv_sem=w_recv.at[k],
            device_id=device(to, partner),
            device_id_type=MESH,
        )

    def copies(name):
        a1, a2, a3 = PIECES[name][3]
        made = {}
        here = dict(at)

        def add(slot, sent, came, to, partner=False):
            made[slot] = (
                lambda: weight_copy(name, slot, sent, to, partner),
                lambda: weight_copy(name, slot, came, to, partner),
            )

        for slot, by in ((0, 1), (1, 3), (2, 2)):
            add(slot, here, {**here, a1: near(a1, -by)}, {a1: near(a1, by)})
        base = 3
        for axis, full, half in ((a2, [a1], a1), (a3, [a1, a2], a1)):
            whole = {**here, **{f: None for f in full}}
            add(base, whole, {**whole, axis: near(axis, -1)}, {axis: near(axis, 1)})
            add(base + 1, whole, {**whole, axis: near(axis, 1)}, {axis: near(axis, -1)})
            first = {**whole, half: ("h", 0)}
            second = {**whole, half: ("h", 1)}
            far = near(axis, 2)
            add(base + 2, {**first, axis: near(axis, -1)}, {**first, axis: far}, {axis: near(axis, 1)})
            add(base + 3, {**second, axis: near(axis, 1)}, {**second, axis: far}, {axis: near(axis, -1)})
            base += 4
        plane = {**here, a1: None, a2: None}
        for slot, by in ((11, 0), (12, 1), (13, 3), (14, 2)):
            sent = {**plane, a3: near(a3, by)}
            add(slot, sent, sent, {}, True)
        return made

    def send(name, *slots):
        for s in slots:
            copies(name)[s][0]().start()

    def came(name, *slots):
        for s in slots:
            copies(name)[s][1]().wait_recv()

    def step(number, name):
        if number == 1:
            send(name, 0, 1, 2)
        elif number == 2:
            came(name, 0, 1, 2)
            send(name, 3, 4)
        elif number == 3:
            came(name, 3, 4)
            send(name, 5, 6)
        elif number == 4:
            came(name, 5, 6)
            send(name, 7, 8, 11)
        elif number == 5:
            came(name, 7, 8)
            send(name, 9, 10, 12, 13)
        elif number == 6:
            came(name, 9, 10)
            send(name, 14)
        else:
            came(name, 11, 12, 13, 14)

    def pump(slot):
        for number, name in planned(slot):
            step(number, name)

    def pump_at(prefix, i, count):
        for k in range(count):
            if planned(f"{prefix}{k}"):
                @pl.when(i == k)
                def _(k=k):
                    pump(f"{prefix}{k}")

    def geometry(b):
        ahead = b < 2
        right = b % 2 == 0
        mine = pl.ds(4, 4) if ahead else pl.ds(0, 4)
        other = pl.ds(0, 4) if ahead else pl.ds(4, 4)
        d_lat = 1 if ahead else -1
        d_lon = 1 if right else -1
        off = 0 if right else 1
        edge = 4 if right else 0
        border = 0 if right else 3
        return mine, other, d_lat, d_lon, off, edge, border

    def halo(b):
        mine, other, d_lat, d_lon, off, edge, border = geometry(b)
        listed = (
            (tok.at[b, other], ext.at[b, other, pl.ds(off, 4)], (-d_lat, 0)),
            (tok.at[b, mine, border], ext.at[b, mine, edge], (0, -d_lon)),
            (tok.at[b, other, border], ext.at[b, other, edge], (-d_lat, -d_lon)),
        )
        return [
            pltpu.make_async_remote_copy(
                src_ref=s, dst_ref=d, send_sem=h_send.at[3 * b + k], recv_sem=h_recv.at[3 * b + k],
                device_id=shifted(*to), device_id_type=MESH,
            )
            for k, (s, d, to) in enumerate(listed)
        ]

    def local_tokens(b):
        mine, _, _, _, off, _, _ = geometry(b)
        return pltpu.make_async_copy(tok.at[b, mine], ext.at[b, mine, pl.ds(off, 4)], t_sem.at[b])

    def returns(b):
        mine, other, d_lat, d_lon, off, edge, _ = geometry(b)
        listed = (
            (back.at[b, other, pl.ds(off, 4)], out.at[b, other], (d_lat, 0)),
            (back.at[b, mine, edge], side.at[b, mine], (0, d_lon)),
            (back.at[b, other, edge], side.at[b, other], (d_lat, d_lon)),
        )
        return [
            pltpu.make_async_remote_copy(
                src_ref=s, dst_ref=d, send_sem=r_send.at[3 * b + k], recv_sem=r_recv.at[3 * b + k],
                device_id=shifted(*to), device_id_type=MESH,
            )
            for k, (s, d, to) in enumerate(listed)
        ]

    def own(which):
        return pltpu.make_async_copy(
            shards[which], held[which].at[z_lo, y, core, z_hi, x], own_sem.at[which]
        )

    for which in range(4):
        own(which).start()
    for b in range(4):
        local_tokens(b).start()

    barrier = pltpu.get_barrier_semaphore()
    peers = [device({a: near(a, by)}) for a in "xyz" for by in (1, 2, 3)]
    peers.append(device({}, True))
    peers += [shifted(i, j) for i in (-1, 0, 1) for j in (-1, 0, 1) if (i, j) != (0, 0)]
    for peer in peers:
        pl.semaphore_signal(barrier, inc=1, device_id=peer, device_id_type=MESH)
    pl.semaphore_wait(barrier, len(peers))

    for which in range(4):
        own(which).wait()
    for n in FIRST:
        step(1, n)
    for b in range(4):
        for c in halo(b):
            c.start()
    for n in LATER:
        step(1, n)

    pump("start")

    early = lax.broadcasted_iota(jnp.int32, (64, D), 0) % 8 < 4

    def window_tokens(b, w):
        left = ext[b, :, w].astype(F32).reshape(64, D)
        right = ext[b, :, w + 1].astype(F32).reshape(64, D)
        return jnp.where(early, right, left)

    def layer_norm(v):
        centre = jnp.mean(v, axis=-1, keepdims=True)
        moved = v - centre
        spread = jnp.mean(moved * moved, axis=-1, keepdims=True)
        return (moved * lax.rsqrt(spread + 1e-05)).astype(BF)

    for b in range(4):
        local_tokens(b).wait()
        for c in halo(b):
            c.wait_recv()

    def norm_one(i, _):
        rows = pl.ds(pl.multiple_of(i * 64, 64), 64)
        normed[rows] = layer_norm(window_tokens(i // 4, i % 4))
        return 0

    lax.fori_loop(0, 16, norm_one, 0)
    pump("norm")

    def qkv_one(i, _):
        pump_at("qkv", i, 4)
        w = wq[i // 2, pl.ds((i % 2) * 2, 2)].reshape(768, D)
        got = lax.dot_general(normed[...], w, (((1,), (1,)), ((), ())), preferred_element_type=F32)
        qkv[:, pl.ds(pl.multiple_of(i * 768, 768), 768)] = got.astype(BF)
        return 0

    lax.fori_loop(0, 4, qkv_one, 0)

    lane_head = lax.broadcasted_iota(jnp.int32, (64, 256), 1) // 64
    pick = [lane_head == h for h in range(4)]
    ones_at = (
        lax.broadcasted_iota(jnp.int32, (256, 256), 0) // 64
        == lax.broadcasted_iota(jnp.int32, (256, 256), 1) // 64
    )
    ones = jnp.where(ones_at, 1.0, 0.0).astype(BF)
    first_half = lax.broadcasted_iota(jnp.int32, (64, 128), 1) < 64
    q_cell = lax.broadcasted_iota(jnp.int32, (64, 128), 0)
    k_cell = lax.broadcasted_iota(jnp.int32, (64, 128), 1) % 64
    itself = q_cell == k_cell
    parted = (q_cell < 32) != (k_cell < 32)

    def spread_heads(v):
        wide = v.astype(F32)
        return jnp.concatenate([jnp.where(p, wide, 0.0).astype(BF) for p in pick], axis=0)

    def attend_one(i, _):
        pump_at("att", i, 16)
        rows = pl.ds(pl.multiple_of(i * 64, 64), 64)
        at_end = jnp.where(i < 8, lat, (lat + 15) % 16) == 15
        end_value = jnp.where(at_end, FAR, 0.0)
        mask = jnp.where(itself, 0.0, jnp.broadcast_to(keys[pl.ds(i, 1)], (64, 128)))
        mask = jnp.where(parted, mask + end_value, mask)
        for g in range(4):
            q = qkv[rows, pl.ds(256 * g, 256)]
            k = qkv[rows, pl.ds(D + 256 * g, 256)]
            v = qkv[rows, pl.ds(2 * D + 256 * g, 256)]
            scores = lax.dot_general(
                q, spread_heads(k), (((1,), (1,)), ((), ())), preferred_element_type=F32
            )
            weights = []
            for t in range(2):
                s = scores[:, 128 * t : 128 * t + 128] * 0.125 + bias[g, :, pl.ds(128 * t, 128)] + mask
                top_a = jnp.max(jnp.where(first_half, s, -jnp.inf), axis=1, keepdims=True)
                top_b = jnp.max(jnp.where(first_half, -jnp.inf, s), axis=1, keepdims=True)
                weights.append(jnp.exp(s - jnp.where(first_half, top_a, top_b)).astype(BF))
            e = jnp.concatenate(weights, axis=1)
            total = jnp.dot(e, ones, preferred_element_type=F32)
            context = jnp.dot(e, spread_heads(v), preferred_element_type=F32) / total
            att[rows, pl.ds(256 * g, 256)] = context.astype(BF)
        return 0

    lax.fori_loop(0, 16, attend_one, 0)

    def proj_one(b, _):
        pump_at("proj", b, 4)
        rows = pl.ds(pl.multiple_of(b * 256, 256), 256)
        got = lax.dot_general(
            att[rows], wp[...].reshape(D, D), (((1,), (1,)), ((), ())), preferred_element_type=F32
        )
        for w in range(4):
            part = pl.ds(pl.multiple_of(b * 256 + w * 64, 64), 64)
            whole = (window_tokens(b, w) + got[64 * w : 64 * w + 64]).astype(BF)
            att[part] = whole
            normed[part] = layer_norm(whole.astype(F32))
        return 0

    lax.fori_loop(0, 4, proj_one, 0)

    def up_one(i, _):
        pump_at("up", i, 8)
        w = wu[i // 4, i % 4].reshape(BLK, D)
        got = lax.dot_general(normed[...], w, (((1,), (1,)), ((), ())), preferred_element_type=F32)
        hid[:, pl.ds(pl.multiple_of(i * BLK, BLK), BLK)] = jax.nn.gelu(got).astype(BF)
        return 0

    lax.fori_loop(0, 8, up_one, 0)
    pump("down0")

    def down_one(b):
        mine, other, _, _, off, edge, _ = geometry(b)
        rows = pl.ds(b * 256, 256)
        got = jnp.dot(hid[rows], wd[...].reshape(4 * D, D), preferred_element_type=F32)
        got = got + att[rows].astype(F32)
        for j in range(5):
            left = got[64 * max(j - 1, 0) : 64 * max(j - 1, 0) + 64]
            right = got[64 * min(j, 3) : 64 * min(j, 3) + 64]
            whole = jnp.where(early, left, right).astype(BF).reshape(8, 8, D)
            back[b, :, j] = whole
            if j != edge:
                out[b, mine, j - off] = whole[4:] if b < 2 else whole[:4]
        for c in returns(b):
            c.start()

    for b in (0, 2, 1, 3):
        down_one(b)

    early_cols = lax.broadcasted_iota(jnp.int32, (64, D), 0) % 8 < 4
    for b in (0, 2, 1, 3):
        border = geometry(b)[6]
        for c in returns(b):
            c.wait_recv()
        here = out[b, :, border].astype(F32).reshape(64, D)
        came_in = side[b].astype(F32).reshape(64, D)
        both = jnp.where(early_cols, came_in, here) if b % 2 == 0 else jnp.where(early_cols, here, came_in)
        out[b, :, border] = both.astype(BF).reshape(8, 8, D)

    for n in NAMES:
        for s in range(PER):
            copies(n)[s][0]().wait_send()
    for b in range(4):
        for c in halo(b) + returns(b):
            c.wait_send()


def window_order(values):
    return jnp.roll(values, (4, 4), axis=(-2, -1)).reshape(values.shape[:-2] + (64,))


def per_device(tokens, qkv_weight, proj_weight, up_weight, down_weight, bias_table, sea_mask):
    head_count = bias_table.shape[1]
    lat = lax.axis_index("lat")
    lon = lax.axis_index("lon")

    cells = window_order(jnp.arange(64, dtype=jnp.int32).reshape(8, 8))
    row_of, col_of = cells // 8, cells % 8
    offsets = (row_of[:, None] - row_of[None, :] + 7) * 15 + (col_of[:, None] - col_of[None, :] + 7)
    one_hot = (offsets.reshape(-1)[:, None] == jnp.arange(bias_table.shape[0], dtype=jnp.int32)).astype(F32)
    bias = jnp.dot(one_hot, bias_table, precision=lax.Precision.HIGHEST)
    bias = bias.reshape(64, 64, head_count // 4, 4).transpose(2, 0, 3, 1).reshape(head_count // 4, 64, 256)

    around = jnp.pad(sea_mask, ((8, 16), (8, 16)), mode="wrap")
    rows = []
    for b in range(4):
        r0 = 8 * (lat if b < 2 else lat - 1) + 8 + 4
        c0 = 32 * lon - (0 if b % 2 == 0 else 8) + 8 + 4
        cut = lax.dynamic_slice(around, (r0, c0), (8, 32))
        rows.append(window_order(cut.reshape(8, 4, 8).transpose(1, 0, 2)))
    keys = jnp.where(jnp.concatenate(rows, axis=0) == 1, 0.0, FAR).astype(F32)
    keys = jnp.concatenate([keys, keys], axis=1)

    hbm = pl.BlockSpec(memory_space=pl.ANY)
    vmem = pl.BlockSpec(memory_space=pltpu.VMEM)
    shard = (2, 4, 2, 2, 4)
    tile = (4, 8, 4, 8, D)
    messages = len(NAMES) * PER
    dma = pltpu.SemaphoreType.DMA
    out = pl.pallas_call(
        block_kernel,
        out_shape=jax.ShapeDtypeStruct(tile, BF),
        in_specs=[hbm] * 5 + [vmem, vmem],
        out_specs=vmem,
        scratch_shapes=[
            pltpu.VMEM(shard + (24, D), BF),
            pltpu.VMEM(shard + (8, D), BF),
            pltpu.VMEM(shard + (32, D), BF),
            pltpu.VMEM(shard + (32, D), BF),
            pltpu.VMEM((4, 8, 5, 8, D), BF),
            pltpu.VMEM((1024, D), BF),
            pltpu.VMEM((1024, 3 * D), BF),
            pltpu.VMEM((1024, D), BF),
            pltpu.VMEM((1024, 4 * D), BF),
            pltpu.VMEM((4, 8, 5, 8, D), BF),
            pltpu.VMEM((4, 8, 8, D), BF),
            dma((messages,)),
            dma((messages,)),
            dma((4,)),
            dma((12,)),
            dma((12,)),
            dma((12,)),
            dma((12,)),
            dma((4,)),
        ],
        compiler_params=pltpu.CompilerParams(
            collective_id=0, has_side_effects=True, vmem_limit_bytes=67043328
        ),
        name="swin_block",
    )(tokens.reshape(tile), qkv_weight, proj_weight, up_weight, down_weight, bias, keys)
    return out.reshape(tokens.shape)


def solution(mesh):
    placed = (
        P(None, "lat", "lon", None),
        P(("lat", "lon"), None),
        P(("lat", "lon"), None),
        P(("lat", "lon"), None),
        P(("lat", "lon"), None),
        P(),
        P(),
    )
    return jax.shard_map(
        per_device,
        mesh=mesh,
        in_specs=placed,
        out_specs=P(None, "lat", "lon", None),
        check_vma=False,
    )
```

```python
import jax
import jax.numpy as jnp
from jax import lax
from jax.experimental import pallas as pl
from jax.experimental.pallas import tpu as pltpu
from jax.sharding import PartitionSpec as P

MESH = pl.DeviceIdType.MESH
BF = jnp.bfloat16
F32 = jnp.float32
D = 1024
BLK = 512
FAR = -1e30

PIECES = {
    "qa": (0, 0, 8, "xyz"),
    "qb": (0, 8, 8, "yzx"),
    "qc": (0, 16, 8, "zxy"),
    "ua": (2, 0, 16, "xyz"),
    "ub": (2, 16, 8, "yzx"),
    "pc": (1, 0, 8, "zxy"),
    "uc": (2, 24, 8, "zxy"),
    "da": (3, 0, 8, "xyz"),
    "db": (3, 8, 16, "yzx"),
    "dc": (3, 24, 8, "zxy"),
}
NAMES = list(PIECES)
PER = 15

PLAN = [
    ("start", 1, "qa"),
    ("start", 1, "qb"),
    ("start", 1, "qc"),
    ("start", 1, "pc"),
    ("start", 1, "ua"),
    ("start", 1, "ub"),
    ("start", 1, "uc"),
    ("start", 1, "da"),
    ("start", 1, "db"),
    ("start", 1, "dc"),
    ("normA", 2, "qa"),
    ("normA", 2, "qb"),
    ("normA", 2, "qc"),
    ("normA", "halo", "columns"),
    ("normA", "halo", "rows"),
    ("normA", 3, "qc"),
    ("normA", 3, "qa"),
    ("normA", 3, "qb"),
    ("normA", 2, "ub"),
    ("normA", 2, "pc"),
    ("normA", 2, "ua"),
    ("normA", 2, "uc"),
    ("normA", 2, "da"),
    ("normA", 2, "db"),
    ("normA", 2, "dc"),
    ("normA", 4, "qb"),
    ("normB", 3, "ub"),
    ("normB", 4, "qc"),
    ("normB", 3, "db"),
    ("normB", 3, "pc"),
    ("normB", 4, "qa"),
    ("qkv0", 3, "uc"),
    ("qkv0", 3, "dc"),
    ("qkv0", 3, "ua"),
    ("qkv0", 3, "da"),
    ("qkv0", 5, "qa"),
    ("qkv0", 5, "qb"),
    ("qkv0", 5, "qc"),
    ("qkv0", 4, "ub"),
    ("qkv0", 4, "pc"),
    ("qkv0", 4, "ua"),
    ("qkv0", 6, "qa"),
    ("qkv0", 6, "qb"),
    ("qkv0", 7, "qa"),
    ("qkv0", 6, "qc"),
    ("qkv0", 7, "qb"),
    ("qkv0", 7, "qc"),
    ("qkv2", 5, "ub"),
    ("qkv2", 4, "db"),
    ("qkv3", 5, "pc"),
    ("qkv3", 4, "uc"),
    ("att2", 5, "ua"),
    ("att2", 6, "ub"),
    ("att2", 4, "da"),
    ("att5", 6, "pc"),
    ("att8", 7, "ub"),
    ("att9", 7, "pc"),
    ("att13", 5, "uc"),
    ("att13", 4, "dc"),
    ("att14", 6, "ua"),
    ("proj2", 7, "ua"),
    ("proj2", 5, "db"),
    ("proj3", 6, "uc"),
    ("up0", 5, "da"),
    ("up0", 7, "uc"),
    ("up2", 5, "dc"),
    ("up3", 6, "da"),
    ("up3", 6, "db"),
    ("up5", 7, "da"),
    ("up5", 7, "db"),
    ("up5", 6, "dc"),
    ("up7", 7, "dc"),
]


def planned(slot):
    return [(what, name) for where, what, name in PLAN if where == slot]


def block_kernel(
    tok, wq_in, wp_in, wu_in, wd_in, table, sea,
    out,
    wq, wp, wu, wd, ext, normed, qkv, att, hid, back, side, spread, bias, keys,
    w_send, w_recv, own_sem, h_send, h_recv, r_send, r_recv, t_sem,
):
    lat = lax.axis_index("lat")
    lon = lax.axis_index("lon")
    core = lat % 2
    y = (lat // 2) % 4
    z_lo = lat // 8
    x = lon % 4
    z_hi = lon // 4
    at = {"x": x, "y": y, "z": z_hi * 2 + z_lo}

    def device(over, partner=False):
        c = dict(at)
        c.update(over)
        k = 1 - core if partner else core
        return {"lat": ((c["z"] % 2) * 4 + c["y"]) * 2 + k, "lon": (c["z"] // 2) * 4 + c["x"]}

    def near(axis, by):
        return (at[axis] + by + 4) % 4

    def shifted(d_lat, d_lon):
        return {"lat": (lat + d_lat + 16) % 16, "lon": (lon + d_lon + 8) % 8}

    held = (wq, wp, wu, wd)
    shards = (wq_in, wp_in, wu_in, wd_in)

    def region(name, c, where):
        which, first, rows, _ = PIECES[name]
        ref = held[which]

        def part(axis):
            v = where[axis]
            if v is None:
                return slice(None)
            if isinstance(v, tuple):
                return pl.ds(2 * v[1], 2)
            return v

        v = where["z"]
        if v is None:
            lo, hi = slice(None), slice(None)
        elif isinstance(v, tuple):
            lo, hi = v[1], slice(None)
        else:
            lo, hi = v % 2, v // 2
        return ref.at[lo, part("y"), c, hi, part("x"), pl.ds(first, rows)]

    def weight_copy(name, slot, where, to, partner=False, src=None):
        k = NAMES.index(name) * PER + slot
        there = region(name, core, where)
        return pltpu.make_async_remote_copy(
            src_ref=there if src is None else src,
            dst_ref=there,
            send_sem=w_send.at[k],
            recv_sem=w_recv.at[k],
            device_id=device(to, partner),
            device_id_type=MESH,
        )

    def copies(name):
        a1, a2, a3 = PIECES[name][3]
        made = {}
        here = dict(at)

        def add(slot, sent, came, to, partner=False):
            made[slot] = (
                lambda: weight_copy(name, slot, sent, to, partner),
                lambda: weight_copy(name, slot, came, to, partner),
            )

        for slot, by in ((0, 1), (1, 3), (2, 2)):
            add(slot, here, {**here, a1: near(a1, -by)}, {a1: near(a1, by)})
        base = 3
        for axis, full, half in ((a2, [a1], a1), (a3, [a1, a2], a1)):
            whole = {**here, **{f: None for f in full}}
            add(base, whole, {**whole, axis: near(axis, -1)}, {axis: near(axis, 1)})
            add(base + 1, whole, {**whole, axis: near(axis, 1)}, {axis: near(axis, -1)})
            first = {**whole, half: ("h", 0)}
            second = {**whole, half: ("h", 1)}
            far = near(axis, 2)
            add(base + 2, {**first, axis: near(axis, -1)}, {**first, axis: far}, {axis: near(axis, 1)})
            add(base + 3, {**second, axis: near(axis, 1)}, {**second, axis: far}, {axis: near(axis, -1)})
            base += 4
        plane = {**here, a1: None, a2: None}
        for slot, by in ((11, 0), (12, 1), (13, 3), (14, 2)):
            sent = {**plane, a3: near(a3, by)}
            add(slot, sent, sent, {}, True)
        return made

    def send(name, *slots):
        for s in slots:
            copies(name)[s][0]().start()

    def came(name, *slots):
        for s in slots:
            copies(name)[s][1]().wait_recv()

    def step(number, name):
        if number == 1:
            send(name, 0, 1, 2)
        elif number == 2:
            came(name, 0, 1, 2)
            send(name, 3, 4)
        elif number == 3:
            came(name, 3, 4)
            send(name, 5, 6)
        elif number == 4:
            came(name, 5, 6)
            send(name, 7, 8, 11)
        elif number == 5:
            came(name, 7, 8)
            send(name, 9, 10, 12, 13)
        elif number == 6:
            came(name, 9, 10)
            send(name, 14)
        else:
            came(name, 11, 12, 13, 14)

    def pump(slot):
        for what, name in planned(slot):
            if what == "halo":
                for b in range(4):
                    for k in (1,) if name == "columns" else (0, 2):
                        halo(b)[k].start()
            else:
                step(what, name)

    def pump_at(prefix, i, count):
        for k in range(count):
            if planned(f"{prefix}{k}"):
                @pl.when(i == k)
                def _(k=k):
                    pump(f"{prefix}{k}")

    def geometry(b):
        ahead = b < 2
        right = b % 2 == 0
        mine = pl.ds(4, 4) if ahead else pl.ds(0, 4)
        other = pl.ds(0, 4) if ahead else pl.ds(4, 4)
        d_lat = 1 if ahead else -1
        d_lon = 1 if right else -1
        off = 0 if right else 1
        edge = 4 if right else 0
        border = 0 if right else 3
        return mine, other, d_lat, d_lon, off, edge, border

    def halo(b):
        mine, other, d_lat, d_lon, off, edge, border = geometry(b)
        listed = (
            (tok.at[b, other], ext.at[b, other, pl.ds(off, 4)], (-d_lat, 0)),
            (tok.at[b, mine, border], ext.at[b, mine, edge], (0, -d_lon)),
            (tok.at[b, other, border], ext.at[b, other, edge], (-d_lat, -d_lon)),
        )
        return [
            pltpu.make_async_remote_copy(
                src_ref=s, dst_ref=d, send_sem=h_send.at[3 * b + k], recv_sem=h_recv.at[3 * b + k],
                device_id=shifted(*to), device_id_type=MESH,
            )
            for k, (s, d, to) in enumerate(listed)
        ]

    def local_tokens(b):
        mine, _, _, _, off, _, _ = geometry(b)
        return pltpu.make_async_copy(tok.at[b, mine], ext.at[b, mine, pl.ds(off, 4)], t_sem.at[b])

    def returns(b):
        mine, other, d_lat, d_lon, off, edge, _ = geometry(b)
        listed = (
            (back.at[b, other, pl.ds(off, 4)], out.at[b, other], (d_lat, 0)),
            (back.at[b, mine, edge], side.at[b, mine], (0, d_lon)),
            (back.at[b, other, edge], side.at[b, other], (d_lat, d_lon)),
        )
        return [
            pltpu.make_async_remote_copy(
                src_ref=s, dst_ref=d, send_sem=r_send.at[3 * b + k], recv_sem=r_recv.at[3 * b + k],
                device_id=shifted(*to), device_id_type=MESH,
            )
            for k, (s, d, to) in enumerate(listed)
        ]

    def own(which):
        return pltpu.make_async_copy(
            shards[which], held[which].at[z_lo, y, core, z_hi, x], own_sem.at[which]
        )

    for which in range(4):
        own(which).start()
    for b in range(4):
        local_tokens(b).start()

    barrier = pltpu.get_barrier_semaphore()
    peers = [device({a: near(a, by)}) for a in "xyz" for by in (1, 2, 3)]
    peers.append(device({}, True))
    peers += [shifted(i, j) for i in (-1, 0, 1) for j in (-1, 0, 1) if (i, j) != (0, 0)]
    for peer in peers:
        pl.semaphore_signal(barrier, inc=1, device_id=peer, device_id_type=MESH)
    pl.semaphore_wait(barrier, len(peers))

    for which in range(4):
        own(which).wait()
    pump("start")

    pump("keys")
    spot = lax.broadcasted_iota(jnp.int32, (256, 512), 1)
    spot_col = spot % 8
    spot_window = spot // 128
    grid_col = lax.broadcasted_iota(jnp.int32, (256, 512), 0)
    own_row = lax.broadcasted_iota(jnp.int32, (8, 512), 0) == (lax.broadcasted_iota(jnp.int32, (8, 512), 1) // 8) % 8
    for b in range(4):
        row = lat if b < 2 else (lat + 15) % 16
        block = lon * 4 + (0 if b % 2 == 0 else 31)
        upper = sea[pl.ds(pl.multiple_of(row * 8, 8), 8)]
        lower = sea[pl.ds(pl.multiple_of(((row + 1) % 16) * 8, 8), 8)]
        band = jnp.concatenate([upper[4:], lower[:4]], axis=0)
        open_at = jnp.where(band == 1, 1.0, 0.0).astype(BF)
        wanted = ((block + spot_window + jnp.where(spot_col < 4, 1, 0)) * 8 + spot_col) % 256
        chosen = jnp.where(grid_col == wanted, 1.0, 0.0).astype(BF)
        found = jnp.dot(open_at, chosen, preferred_element_type=F32)
        found = jnp.sum(jnp.where(own_row, found, 0.0), axis=0, keepdims=True)
        closed = jnp.where(found > 0.5, 0.0, FAR)
        for w in range(4):
            keys[4 * b + w : 4 * b + w + 1] = closed[:, 128 * w : 128 * w + 128]

    pump("bias")
    lane = lax.broadcasted_iota(jnp.int32, (16, 256), 1)
    head_row = lax.broadcasted_iota(jnp.int32, (16, 256), 0)
    lane_row = (lane % 64) // 8
    col_step = (lax.broadcasted_iota(jnp.int32, (8, 256), 0) + 4) % 8 - (
        lax.broadcasted_iota(jnp.int32, (8, 256), 1) + 4
    ) % 8 + 7
    for g in range(4):
        over_lanes = jnp.where(head_row == 4 * g + lane // 64, 1.0, 0.0)
        wide = jnp.dot(
            table[...], over_lanes, precision=lax.Precision.HIGHEST, preferred_element_type=F32
        )
        for d in range(15):
            spread[g, d, 0:15] = wide[15 * d : 15 * d + 15]

    def bias_one(i, _):
        g, r = i // 8, i % 8
        steps = jnp.zeros((16, 256), F32)
        for k in range(8):
            steps = jnp.where(lane_row == k, spread[g, r - k + 7], steps)
        line = jnp.zeros((8, 256), F32)
        for d in range(15):
            line = jnp.where(col_step == d, steps[d : d + 1], line)
        bias[g, pl.ds(pl.multiple_of(r * 8, 8), 8)] = line
        return 0

    lax.fori_loop(0, 32, bias_one, 0)

    early = lax.broadcasted_iota(jnp.int32, (32, D), 0) % 8 < 4

    def window_half(b, w, half):
        rows = pl.ds(jnp.where((b < 2) == (half == 0), 4, 0), 4)
        left = ext[b, rows, w].astype(F32).reshape(32, D)
        right = ext[b, rows, w + 1].astype(F32).reshape(32, D)
        return jnp.where(early, right, left)

    def layer_norm(v):
        centre = jnp.mean(v, axis=-1, keepdims=True)
        moved = v - centre
        spread_of = jnp.mean(moved * moved, axis=-1, keepdims=True)
        return (moved * lax.rsqrt(spread_of + 1e-05)).astype(BF)

    def norm_half(half):
        def norm_one(i, _):
            rows = pl.ds(pl.multiple_of(half * 512 + i * 32, 32), 32)
            normed[rows] = layer_norm(window_half(i // 4, i % 4, half))
            return 0

        lax.fori_loop(0, 16, norm_one, 0)

    pump("normA")
    for b in range(4):
        local_tokens(b).wait()
        halo(b)[1].wait_recv()
    norm_half(0)
    pump("normB")
    for b in range(4):
        halo(b)[0].wait_recv()
        halo(b)[2].wait_recv()
    norm_half(1)

    def qkv_one(i, _):
        pump_at("qkv", i, 4)
        w = wq[i // 2, pl.ds((i % 2) * 2, 2)].reshape(768, D)
        got = lax.dot_general(normed[...], w, (((1,), (1,)), ((), ())), preferred_element_type=F32)
        qkv[:, pl.ds(pl.multiple_of(i * 768, 768), 768)] = got.astype(BF)
        return 0

    lax.fori_loop(0, 4, qkv_one, 0)

    lane_head = lax.broadcasted_iota(jnp.int32, (64, 256), 1) // 64
    pick = [lane_head == h for h in range(4)]
    ones_at = (
        lax.broadcasted_iota(jnp.int32, (256, 256), 0) // 64
        == lax.broadcasted_iota(jnp.int32, (256, 256), 1) // 64
    )
    ones = jnp.where(ones_at, 1.0, 0.0).astype(BF)
    first_half = lax.broadcasted_iota(jnp.int32, (64, 128), 1) < 64
    q_cell = lax.broadcasted_iota(jnp.int32, (64, 128), 0)
    k_cell = lax.broadcasted_iota(jnp.int32, (64, 128), 1) % 64
    itself = q_cell == k_cell
    parted = (q_cell < 32) != (k_cell < 32)

    def spread_heads(v):
        wide = v.astype(F32)
        return jnp.concatenate([jnp.where(p, wide, 0.0).astype(BF) for p in pick], axis=0)

    def attend_one(i, _):
        pump_at("att", i, 16)
        flip = jnp.where(i < 8, 0, 512)
        top = pl.ds(pl.multiple_of(flip + i * 32, 32), 32)
        low = pl.ds(pl.multiple_of(512 - flip + i * 32, 32), 32)

        def cut(first):
            return jnp.concatenate([qkv[top, pl.ds(first, 256)], qkv[low, pl.ds(first, 256)]], axis=0)

        at_end = jnp.where(i < 8, lat, (lat + 15) % 16) == 15
        end_value = jnp.where(at_end, FAR, 0.0)
        mask = jnp.where(itself, 0.0, jnp.broadcast_to(keys[pl.ds(i, 1)], (64, 128)))
        mask = jnp.where(parted, mask + end_value, mask)
        for g in range(4):
            q, k, v = cut(256 * g), cut(D + 256 * g), cut(2 * D + 256 * g)
            scores = lax.dot_general(
                q, spread_heads(k), (((1,), (1,)), ((), ())), preferred_element_type=F32
            )
            weights = []
            for t in range(2):
                s = scores[:, 128 * t : 128 * t + 128] * 0.125 + bias[g, :, pl.ds(128 * t, 128)] + mask
                top_a = jnp.max(jnp.where(first_half, s, -jnp.inf), axis=1, keepdims=True)
                top_b = jnp.max(jnp.where(first_half, -jnp.inf, s), axis=1, keepdims=True)
                weights.append(jnp.exp(s - jnp.where(first_half, top_a, top_b)).astype(BF))
            e = jnp.concatenate(weights, axis=1)
            total = jnp.dot(e, ones, preferred_element_type=F32)
            context = jnp.dot(e, spread_heads(v), preferred_element_type=F32) / total
            att[top, pl.ds(256 * g, 256)] = context[:32].astype(BF)
            att[low, pl.ds(256 * g, 256)] = context[32:].astype(BF)
        return 0

    lax.fori_loop(0, 16, attend_one, 0)

    def proj_one(i, _):
        pump_at("proj", i, 4)
        rows = pl.ds(pl.multiple_of(i * 256, 256), 256)
        got = lax.dot_general(
            att[rows], wp[...].reshape(D, D), (((1,), (1,)), ((), ())), preferred_element_type=F32
        )
        for w in range(8):
            part = pl.ds(pl.multiple_of(i * 256 + w * 32, 32), 32)
            before = window_half((i % 2) * 2 + w // 4, w % 4, i // 2)
            whole = (before + got[32 * w : 32 * w + 32]).astype(BF)
            att[part] = whole
            normed[part] = layer_norm(whole.astype(F32))
        return 0

    lax.fori_loop(0, 4, proj_one, 0)

    def up_one(i, _):
        pump_at("up", i, 8)
        w = wu[i // 4, i % 4].reshape(BLK, D)
        got = lax.dot_general(normed[...], w, (((1,), (1,)), ((), ())), preferred_element_type=F32)
        hid[:, pl.ds(pl.multiple_of(i * BLK, BLK), BLK)] = jax.nn.gelu(got).astype(BF)
        return 0

    lax.fori_loop(0, 8, up_one, 0)
    pump("down0")

    def down_one(i):
        half = i // 2
        got = jnp.dot(hid[256 * i : 256 * i + 256], wd[...].reshape(4 * D, D), preferred_element_type=F32)
        got = got + att[256 * i : 256 * i + 256].astype(F32)
        for b in (2 * (i % 2), 2 * (i % 2) + 1):
            mine, other, _, _, off, edge, _ = geometry(b)
            base = 128 * (b % 2)
            for j in range(5):
                left = got[base + 32 * max(j - 1, 0) : base + 32 * max(j - 1, 0) + 32]
                right = got[base + 32 * min(j, 3) : base + 32 * min(j, 3) + 32]
                whole = jnp.where(early, left, right).astype(BF).reshape(4, 8, D)
                if half == 1:
                    back[b, other, j] = whole
                elif j == edge:
                    back[b, mine, j] = whole
                else:
                    out[b, mine, j - off] = whole
            for k in (0, 2) if half == 1 else (1,):
                returns(b)[k].start()

    for i in (2, 3, 0, 1):
        down_one(i)

    early_cols = lax.broadcasted_iota(jnp.int32, (64, D), 0) % 8 < 4
    for b in range(4):
        border = geometry(b)[6]
        for c in returns(b):
            c.wait_recv()
        here = out[b, :, border].astype(F32).reshape(64, D)
        came_in = side[b].astype(F32).reshape(64, D)
        both = jnp.where(early_cols, came_in, here) if b % 2 == 0 else jnp.where(early_cols, here, came_in)
        out[b, :, border] = both.astype(BF).reshape(8, 8, D)

    for n in NAMES:
        for s in range(PER):
            copies(n)[s][0]().wait_send()
    for b in range(4):
        for c in halo(b) + returns(b):
            c.wait_send()


def per_device(tokens, qkv_weight, proj_weight, up_weight, down_weight, bias_table, sea_mask):
    hbm = pl.BlockSpec(memory_space=pl.ANY)
    vmem = pl.BlockSpec(memory_space=pltpu.VMEM)
    shard = (2, 4, 2, 2, 4)
    tile = (4, 8, 4, 8, D)
    messages = len(NAMES) * PER
    dma = pltpu.SemaphoreType.DMA
    out = pl.pallas_call(
        block_kernel,
        out_shape=jax.ShapeDtypeStruct(tile, BF),
        in_specs=[hbm] * 5 + [vmem, vmem],
        out_specs=vmem,
        scratch_shapes=[
            pltpu.VMEM(shard + (24, D), BF),
            pltpu.VMEM(shard + (8, D), BF),
            pltpu.VMEM(shard + (32, D), BF),
            pltpu.VMEM(shard + (32, D), BF),
            pltpu.VMEM((4, 8, 5, 8, D), BF),
            pltpu.VMEM((1024, D), BF),
            pltpu.VMEM((1024, 3 * D), BF),
            pltpu.VMEM((1024, D), BF),
            pltpu.VMEM((1024, 4 * D), BF),
            pltpu.VMEM((4, 8, 5, 8, D), BF),
            pltpu.VMEM((4, 8, 8, D), BF),
            pltpu.VMEM((4, 15, 16, 256), F32),
            pltpu.VMEM((4, 64, 256), F32),
            pltpu.VMEM((16, 128), F32),
            dma((messages,)),
            dma((messages,)),
            dma((4,)),
            dma((12,)),
            dma((12,)),
            dma((12,)),
            dma((12,)),
            dma((4,)),
        ],
        compiler_params=pltpu.CompilerParams(
            collective_id=0, has_side_effects=True, vmem_limit_bytes=67043328
        ),
        name="swin_block",
    )(tokens.reshape(tile), qkv_weight, proj_weight, up_weight, down_weight, bias_table, sea_mask)
    return out.reshape(tokens.shape)


def solution(mesh):
    placed = (
        P(None, "lat", "lon", None),
        P(("lat", "lon"), None),
        P(("lat", "lon"), None),
        P(("lat", "lon"), None),
        P(("lat", "lon"), None),
        P(),
        P(),
    )
    return jax.shard_map(
        per_device,
        mesh=mesh,
        in_specs=placed,
        out_specs=P(None, "lat", "lon", None),
        check_vma=False,
    )
```

```python
import jax
import jax.numpy as jnp
from jax import lax
from jax.experimental import pallas as pl
from jax.experimental.pallas import tpu as pltpu
from jax.sharding import PartitionSpec as P

MESH = pl.DeviceIdType.MESH
BF = jnp.bfloat16
F32 = jnp.float32
D = 1024
FAR = -1e30

PIECES = {
    "qa": (0, 0, 0, 1024, "xyz"),
    "qb": (0, 8, 0, 1024, "yzx"),
    "qc": (0, 16, 0, 1024, "zxy"),
    "p": (1, 0, 0, 1024, "xyz"),
    "c0a": (2, 0, 0, 384, "yzx"),
    "c0b": (2, 0, 384, 384, "zxy"),
    "c0c": (2, 0, 768, 256, "xyz"),
    "c1a": (2, 1, 0, 384, "yzx"),
    "c1b": (2, 1, 384, 384, "zxy"),
    "c1c": (2, 1, 768, 256, "xyz"),
    "c2a": (2, 2, 0, 384, "yzx"),
    "c2b": (2, 2, 384, 384, "zxy"),
    "c2c": (2, 2, 768, 256, "xyz"),
    "c3a": (2, 3, 0, 384, "yzx"),
    "c3b": (2, 3, 384, 384, "zxy"),
    "c3c": (2, 3, 768, 256, "xyz"),
}
NAMES = list(PIECES)
FINE = ("qa", "qb", "qc")
COUNT = {n: 27 if n in FINE else 15 for n in NAMES}
START = {n: sum(COUNT[m] for m in NAMES[:k]) for k, n in enumerate(NAMES)}
FINE_STEPS = {
    1: ((), (0, 1, 2)),
    2: ((0, 1, 2), (3, 4, 7, 8)),
    3: ((3, 4), (5, 6, 11, 12, 15, 16)),
    4: ((5, 6), (19, 20, 23)),
    5: ((7, 8), (9, 10)),
    6: ((11, 12, 15, 16), (13, 14, 17, 18)),
    7: ((19, 20), (21, 22, 24, 25)),
    8: ((9, 10, 13, 14, 17, 18, 21, 22), (26,)),
    9: ((23, 24, 25, 26), ()),
}
STEPS = {
    1: ((), (0, 1, 2)),
    2: ((0, 1, 2), (3, 4)),
    3: ((3, 4), (5, 6)),
    4: ((5, 6), (7, 8, 11)),
    5: ((7, 8), (9, 10, 12, 13)),
    6: ((9, 10), (14,)),
    7: ((11, 12, 13, 14), ()),
}
PLAN = [
    ("start", 1, "qa"),
    ("start", 1, "qb"),
    ("start", 1, "qc"),
    ("start", "halo", 1),
    ("start", "halo", 3),
    ("start", "halo", 5),
    ("normA", 2, "qa"),
    ("normA", 2, "qb"),
    ("normA", 2, "qc"),
    ("normA", "halo", 4),
    ("normA", "halo", 0),
    ("normA", "halo", 2),
    ("normA", 3, "qa"),
    ("normA", 3, "qb"),
    ("normA", 3, "qc"),
    ("normA", 1, "p"),
    ("normA", 1, "c0a"),
    ("normA", 1, "c0b"),
    ("normA", 1, "c0c"),
    ("normA", 1, "c1a"),
    ("normA", 1, "c1b"),
    ("normA", 1, "c1c"),
    ("normA", 1, "c2a"),
    ("normA", 1, "c2b"),
    ("normA", 1, "c2c"),
    ("normA", 1, "c3a"),
    ("normA", 1, "c3b"),
    ("normA", 1, "c3c"),
    ("normB", 4, "qa"),
    ("normB", 5, "qa"),
    ("normB", 6, "qa"),
    ("qkv0", 4, "qb"),
    ("qkv0", 4, "qc"),
    ("qkv0", 2, "c0b"),
    ("qkv0", 5, "qb"),
    ("qkv0", 5, "qc"),
    ("qkv0", 6, "qb"),
    ("qkv0", 6, "qc"),
    ("qkv0", 2, "c1b"),
    ("qkv0", 2, "p"),
    ("qkv0", 2, "c0a"),
    ("qkv0", 2, "c2b"),
    ("qkv0", 2, "c0c"),
    ("qkv0", 2, "c1a"),
    ("qkv0", 2, "c1c"),
    ("qkv0", 2, "c3b"),
    ("qkv0", 2, "c2c"),
    ("qkv0", 2, "c2a"),
    ("qkv0", 7, "qa"),
    ("qkv0", 2, "c3c"),
    ("qkv0", 2, "c3a"),
    ("qkv0", 7, "qb"),
    ("qkv0", 7, "qc"),
    ("qkv0", 3, "c0b"),
    ("qkv0", 3, "c0a"),
    ("qkv0", 3, "c1a"),
    ("qkv0", 3, "p"),
    ("qkv0", 3, "c2a"),
    ("qkv0", 3, "c1b"),
    ("qkv0", 3, "c0c"),
    ("qkv0", 8, "qa"),
    ("qkv0", 3, "c1c"),
    ("qkv0", 3, "c2b"),
    ("qkv0", 3, "c3a"),
    ("qkv0", 3, "c2c"),
    ("qkv0", 4, "c0a"),
    ("qkv0", 9, "qa"),
    ("qkv0", 3, "c3b"),
    ("qkv0", 3, "c3c"),
    ("qkv0", 4, "c1a"),
    ("qkv0", 8, "qb"),
    ("qkv0", 8, "qc"),
    ("qkv0", 4, "c0b"),
    ("qkv0", 4, "p"),
    ("qkv0", 4, "c1b"),
    ("qkv0", 4, "c0c"),
    ("qkv0", 9, "qb"),
    ("qkv0", 9, "qc"),
    ("qkv3", 5, "c0a"),
    ("qkv3", 4, "c2a"),
    ("att0", 5, "c0b"),
    ("att0", 4, "c2b"),
    ("att1", 5, "p"),
    ("att1", 4, "c1c"),
    ("att3", 5, "c1a"),
    ("att3", 4, "c3a"),
    ("att5", 5, "c1b"),
    ("att5", 4, "c3b"),
    ("att5", 5, "c0c"),
    ("att5", 4, "c2c"),
    ("att7", 6, "c0a"),
    ("att9", 6, "c0b"),
    ("att11", 7, "c0a"),
    ("att12", 6, "p"),
    ("att13", 7, "c0b"),
    ("att14", 5, "c2a"),
    ("proj0", 7, "p"),
    ("proj0", 5, "c1c"),
    ("proj0", 4, "c3c"),
    ("proj0", 5, "c2b"),
    ("proj1", 6, "c1a"),
    ("proj2", 6, "c0c"),
    ("proj2", 6, "c1b"),
    ("proj3", 7, "c1a"),
    ("big0", 7, "c0c"),
    ("big0", 7, "c1b"),
    ("big0", 5, "c2c"),
    ("big1", 6, "c1c"),
    ("big1", 6, "c2a"),
    ("big1", 5, "c3a"),
    ("big1", 5, "c3b"),
    ("big1", 5, "c3c"),
    ("big1", 6, "c2b"),
    ("big1", 7, "c1c"),
    ("big2", 7, "c2a"),
    ("big2", 7, "c2b"),
    ("big2", 6, "c2c"),
    ("big2", 6, "c3c"),
    ("big2", 6, "c3a"),
    ("big2", 6, "c3b"),
    ("big2", 7, "c2c"),
    ("big3", 7, "c3a"),
    ("big3", 7, "c3b"),
    ("big3", 7, "c3c"),
]


def planned(slot):
    return [(what, name) for where, what, name in PLAN if where == slot]


def block_kernel(
    tok, wq_in, wp_in, wu_in, wd_in, table, sea,
    out, side,
    wq, wp, wf, ext, normed, qkv, att, acc, back, spread, bias, keys,
    w_send, w_recv, own_sem, h_send, h_recv, r_send, r_recv, t_sem, o_sem,
):
    lat = lax.axis_index("lat")
    lon = lax.axis_index("lon")
    core = lat % 2
    y = (lat // 2) % 4
    z_lo = lat // 8
    x = lon % 4
    z_hi = lon // 4
    at = {"x": x, "y": y, "z": z_hi * 2 + z_lo}

    def device(over, partner=False):
        c = dict(at)
        c.update(over)
        k = 1 - core if partner else core
        return {"lat": ((c["z"] % 2) * 4 + c["y"]) * 2 + k, "lon": (c["z"] // 2) * 4 + c["x"]}

    ring = {a: [at[a]] + [(at[a] + by) % 4 for by in (1, 2, 3)] for a in "xyz"}

    def near(axis, by):
        return ring[axis][by % 4]

    def shifted(d_lat, d_lon):
        return {"lat": (lat + d_lat + 16) % 16, "lon": (lon + d_lon + 8) % 8}

    held = (wq, wp, wf)

    def region(name, c, where):
        which, first, col, cols, _ = PIECES[name]
        ref = held[which]

        def part(axis):
            v = where[axis]
            if v is None:
                return slice(None)
            if isinstance(v, tuple):
                return pl.ds(2 * v[1], 2)
            return v

        v = where["z"]
        if v is None:
            lo, hi = slice(None), slice(None)
        elif isinstance(v, tuple):
            lo, hi = v[1], slice(None)
        else:
            lo, hi = v % 2, v // 2
        rows = (first, slice(None)) if which == 2 else (pl.ds(first, 8),)
        return ref.at[(lo, part("y"), c, hi, part("x"), *rows, pl.ds(col, cols))]

    targets = {(a, by): device({a: near(a, by)}) for a in "xyz" for by in (1, 2, 3)}
    partner = device({}, True)

    def message(name, m):
        a1, a2, a3 = PIECES[name][4]
        here = dict(at)
        if m < 3:
            by = (1, 3, 2)[m]
            return here, {**here, a1: near(a1, -by)}, targets[a1, by]
        m -= 3
        line = {**here, a1: None}
        plane = {**line, a2: None}
        if m < 4:
            axis, whole = a2, line
        elif name in FINE and m < 20:
            axis, whole = a3, {**line, a2: near(a2, (0, 3, 1, 2)[(m - 4) // 4])}
        elif m < 8:
            axis, whole = a3, plane
        else:
            by = (0, 1, 3, 2)[m - (20 if name in FINE else 8)]
            sent = {**plane, a3: near(a3, by)}
            return sent, sent, partner
        m %= 4
        if m < 2:
            by = 1 if m == 0 else 3
            return whole, {**whole, axis: near(axis, -by)}, targets[axis, by]
        by = 1 if m == 2 else 3
        half = {**whole, a1: ("h", m - 2)}
        return {**half, axis: near(axis, -by)}, {**half, axis: near(axis, 2)}, targets[axis, by]

    def weight_copy(name, m, where, to):
        k = START[name] + m
        there = region(name, core, where)
        return pltpu.make_async_remote_copy(
            src_ref=there, dst_ref=there, send_sem=w_send.at[k], recv_sem=w_recv.at[k],
            device_id=to, device_id_type=MESH,
        )

    def send(name, m):
        sent, _, to = message(name, m)
        return weight_copy(name, m, sent, to)

    def came(name, m):
        _, landed, to = message(name, m)
        return weight_copy(name, m, landed, to)

    def step(number, name):
        awaited, sent = (FINE_STEPS if name in FINE else STEPS)[number]
        for m in awaited:
            came(name, m).wait_recv()
        for m in sent:
            send(name, m).start()

    def pump(slot):
        for what, name in planned(slot):
            if what == "halo":
                for b in (0, 2, 1, 3):
                    halo(b, name).start()
            else:
                step(what, name)

    def pump_at(prefix, i, count):
        for k in range(count):
            if planned(f"{prefix}{k}"):
                @pl.when(i == (k - k % 2 if prefix == "att" else k))
                def _(k=k):
                    pump(f"{prefix}{k}")

    def geometry(b):
        ahead = b < 2
        right = b % 2 == 0
        mine = pl.ds(4, 4) if ahead else pl.ds(0, 4)
        other = pl.ds(0, 4) if ahead else pl.ds(4, 4)
        d_lat = 1 if ahead else -1
        d_lon = 1 if right else -1
        off = 0 if right else 1
        edge = 4 if right else 0
        border = 0 if right else 3
        return mine, other, d_lat, d_lon, off, edge, border

    def halo(b, k):
        _, other, d_lat, d_lon, off, edge, border = geometry(b)
        mine_first, other_first = (4, 0) if b < 2 else (0, 4)
        mine = pl.ds(mine_first, 4)
        if k < 4:
            src, dst = tok.at[b, other_first + k], ext.at[b, other_first + k, pl.ds(off, 4)]
            to = shifted(-d_lat, 0)
        elif k == 4:
            src, dst, to = tok.at[b, mine, border], ext.at[b, mine, edge], shifted(0, -d_lon)
        else:
            src, dst, to = tok.at[b, other, border], ext.at[b, other, edge], shifted(-d_lat, -d_lon)
        return pltpu.make_async_remote_copy(
            src_ref=src, dst_ref=dst, send_sem=h_send.at[6 * b + k], recv_sem=h_recv.at[6 * b + k],
            device_id=to, device_id_type=MESH,
        )

    def local_tokens(b):
        mine, _, _, _, off, _, _ = geometry(b)
        return pltpu.make_async_copy(tok.at[b, mine], ext.at[b, mine, pl.ds(off, 4)], t_sem.at[b])

    def returns(b, k):
        mine, other, d_lat, d_lon, off, edge, _ = geometry(b)
        src, dst, to = (
            (back.at[b, other, pl.ds(off, 4)], out.at[b, other], (d_lat, 0)),
            (back.at[b, mine, edge], side.at[b, mine], (0, d_lon)),
            (back.at[b, other, edge], side.at[b, other], (d_lat, d_lon)),
        )[k]
        return pltpu.make_async_remote_copy(
            src_ref=src, dst_ref=dst, send_sem=r_send.at[3 * b + k], recv_sem=r_recv.at[3 * b + k],
            device_id=shifted(*to), device_id_type=MESH,
        )

    def own(which):
        here = (z_lo, y, core, z_hi, x)
        src, dst = (
            (wq_in, wq.at[here]),
            (wp_in, wp.at[here]),
            (wu_in, wf.at[(*here, slice(None), pl.ds(0, 8))]),
            (wd_in, wf.at[(*here, slice(None), pl.ds(8, 8))]),
        )[which]
        return pltpu.make_async_copy(src, dst, own_sem.at[which])

    for which in range(4):
        own(which).start()
    for b in range(4):
        local_tokens(b).start()

    barrier = pltpu.get_barrier_semaphore()
    peers = list(targets.values()) + [partner]
    peers += [shifted(i, j) for i in (-1, 0, 1) for j in (-1, 0, 1) if (i, j) != (0, 0)]
    for peer in peers:
        pl.semaphore_signal(barrier, inc=1, device_id=peer, device_id_type=MESH)
    pl.semaphore_wait(barrier, len(peers))

    for which in range(4):
        own(which).wait()
    pump("start")

    pump("keys")
    spot = lax.broadcasted_iota(jnp.int32, (256, 512), 1)
    spot_col = spot % 8
    spot_window = spot // 128
    grid_col = lax.broadcasted_iota(jnp.int32, (256, 512), 0)
    own_row = lax.broadcasted_iota(jnp.int32, (8, 512), 0) == (lax.broadcasted_iota(jnp.int32, (8, 512), 1) // 8) % 8
    for b in range(4):
        row = lat if b < 2 else (lat + 15) % 16
        block = lon * 4 + (0 if b % 2 == 0 else 31)
        upper = sea[pl.ds(pl.multiple_of(row * 8, 8), 8)]
        lower = sea[pl.ds(pl.multiple_of(((row + 1) % 16) * 8, 8), 8)]
        band = jnp.concatenate([upper[4:], lower[:4]], axis=0)
        open_at = jnp.where(band == 1, 1.0, 0.0).astype(BF)
        wanted = ((block + spot_window + jnp.where(spot_col < 4, 1, 0)) * 8 + spot_col) % 256
        chosen = jnp.where(grid_col == wanted, 1.0, 0.0).astype(BF)
        found = jnp.dot(open_at, chosen, preferred_element_type=F32)
        found = jnp.sum(jnp.where(own_row, found, 0.0), axis=0, keepdims=True)
        closed = jnp.where(found > 0.5, 0.0, FAR)
        for w in range(4):
            keys[4 * b + w : 4 * b + w + 1] = closed[:, 128 * w : 128 * w + 128]

    pump("bias")
    lane = lax.broadcasted_iota(jnp.int32, (16, 256), 1)
    head_row = lax.broadcasted_iota(jnp.int32, (16, 256), 0)
    lane_row = (lane % 64) // 8
    col_step = (lax.broadcasted_iota(jnp.int32, (8, 256), 0) + 4) % 8 - (
        lax.broadcasted_iota(jnp.int32, (8, 256), 1) + 4
    ) % 8 + 7
    for g in range(4):
        over_lanes = jnp.where(head_row == 4 * g + lane // 64, 1.0, 0.0)
        wide = jnp.dot(
            table[...], over_lanes, precision=lax.Precision.HIGHEST, preferred_element_type=F32
        )
        for d in range(15):
            spread[g, d, 0:15] = wide[15 * d : 15 * d + 15]

    def bias_one(i, _):
        g, r = i // 8, i % 8
        steps = jnp.zeros((16, 256), F32)
        for k in range(8):
            steps = jnp.where(lane_row == k, spread[g, r - k + 7], steps)
        line = jnp.zeros((8, 256), F32)
        for d in range(15):
            line = jnp.where(col_step == d, steps[d : d + 1], line)
        bias[g, pl.ds(pl.multiple_of(r * 8, 8), 8)] = line
        return 0

    lax.fori_loop(0, 32, bias_one, 0)

    def other_row(b, w):
        return 512 + 128 * ((b + 2 * core) % 4) + 32 * w

    def own_row(b, w):
        if isinstance(b, int):
            edge_here = w == (3 if b % 2 == 0 else 0)
            return 384 + 32 * b if edge_here else 32 * (3 * b + w - b % 2)
        odd = b % 2
        edge_here = w == 3 - 3 * odd
        return jnp.where(edge_here, 384 + 32 * b, 32 * (3 * b + w - odd))

    early = lax.broadcasted_iota(jnp.int32, (32, D), 0) % 8 < 4

    def window_half(b, w, half):
        rows = pl.ds(jnp.where((b < 2) == (half == 0), 4, 0), 4)
        left = ext[b, rows, w].astype(F32).reshape(32, D)
        right = ext[b, rows, w + 1].astype(F32).reshape(32, D)
        return jnp.where(early, right, left)

    def layer_norm(v):
        centre = jnp.mean(v, axis=-1, keepdims=True)
        moved = v - centre
        spread_of = jnp.mean(moved * moved, axis=-1, keepdims=True)
        return (moved * lax.rsqrt(spread_of + 1e-05)).astype(BF)

    def norm_half(half):
        def norm_one(i, _):
            first = (other_row if half else own_row)(i // 4, i % 4)
            rows = pl.ds(pl.multiple_of(first, 32), 32)
            normed[rows] = layer_norm(window_half(i // 4, i % 4, half))
            return 0

        lax.fori_loop(0, 16, norm_one, 0)

    pump("normA")
    for b in range(4):
        local_tokens(b).wait()
        halo(b, 4).wait_recv()
    norm_half(0)
    pump("normB")
    for b in range(4):
        for k in (0, 1, 2, 3, 5):
            halo(b, k).wait_recv()
    norm_half(1)

    def qkv_one(i, _):
        pump_at("qkv", i, 4)
        w = wq[i // 2, pl.ds((i % 2) * 2, 2)].reshape(768, D)
        got = lax.dot_general(normed[...], w, (((1,), (1,)), ((), ())), preferred_element_type=F32)
        qkv[:, pl.ds(pl.multiple_of(i * 768, 768), 768)] = got.astype(BF)
        return 0

    lax.fori_loop(0, 4, qkv_one, 0)

    lane_head = lax.broadcasted_iota(jnp.int32, (64, 256), 1) // 64
    pick = [lane_head == h for h in range(4)]
    ones_at = (
        lax.broadcasted_iota(jnp.int32, (256, 256), 0) // 64
        == lax.broadcasted_iota(jnp.int32, (256, 256), 1) // 64
    )
    ones = jnp.where(ones_at, 1.0, 0.0).astype(BF)
    first_half = lax.broadcasted_iota(jnp.int32, (64, 128), 1) < 64
    q_cell = lax.broadcasted_iota(jnp.int32, (64, 128), 0)
    k_cell = lax.broadcasted_iota(jnp.int32, (64, 128), 1) % 64
    itself = q_cell == k_cell
    parted = (q_cell < 32) != (k_cell < 32)

    def spread_heads(v):
        wide = v.astype(F32)
        return jnp.concatenate([jnp.where(p, wide, 0.0).astype(BF) for p in pick], axis=0)

    def attend_one(i, _):
        owned, foreign = own_row(i // 4, i % 4), other_row(i // 4, i % 4)
        top = pl.ds(pl.multiple_of(jnp.where(i < 8, owned, foreign), 32), 32)
        low = pl.ds(pl.multiple_of(jnp.where(i < 8, foreign, owned), 32), 32)

        def cut(first):
            return jnp.concatenate([qkv[top, pl.ds(first, 256)], qkv[low, pl.ds(first, 256)]], axis=0)

        at_end = jnp.where(i < 8, lat, (lat + 15) % 16) == 15
        end_value = jnp.where(at_end, FAR, 0.0)
        mask = jnp.where(itself, 0.0, jnp.broadcast_to(keys[pl.ds(i, 1)], (64, 128)))
        mask = jnp.where(parted, mask + end_value, mask)
        for g in range(4):
            q, k, v = cut(256 * g), cut(D + 256 * g), cut(2 * D + 256 * g)
            scores = lax.dot_general(
                q, spread_heads(k), (((1,), (1,)), ((), ())), preferred_element_type=F32
            )
            weights = []
            for t in range(2):
                s = scores[:, 128 * t : 128 * t + 128] * 0.125 + bias[g, :, pl.ds(128 * t, 128)] + mask
                top_a = jnp.max(jnp.where(first_half, s, -jnp.inf), axis=1, keepdims=True)
                top_b = jnp.max(jnp.where(first_half, -jnp.inf, s), axis=1, keepdims=True)
                weights.append(jnp.exp(s - jnp.where(first_half, top_a, top_b)).astype(BF))
            e = jnp.concatenate(weights, axis=1)
            total = jnp.dot(e, ones, preferred_element_type=F32)
            context = jnp.dot(e, spread_heads(v), preferred_element_type=F32) / total
            att[top, pl.ds(256 * g, 256)] = context[:32].astype(BF)
            att[low, pl.ds(256 * g, 256)] = context[32:].astype(BF)
        return 0

    def attend_two(i, _):
        pump_at("att", i * 2, 16)
        attend_one(i * 2, 0)
        attend_one(i * 2 + 1, 0)
        return 0

    lax.fori_loop(0, 8, attend_two, 0)

    def proj_one(i, _):
        pump_at("proj", i, 4)
        rows = pl.ds(pl.multiple_of(i * 256, 256), 256)
        got = lax.dot_general(
            att[rows], wp[...].reshape(D, D), (((1,), (1,)), ((), ())), preferred_element_type=F32
        )
        for w in range(8):
            part = pl.ds(pl.multiple_of(i * 256 + w * 32, 32), 32)
            slot = i * 8 + w
            edge_b = jnp.clip(slot - 12, 0, 3)
            inner_b = jnp.minimum(slot // 3, 3)
            b = jnp.where(slot < 12, inner_b, jnp.where(slot < 16, edge_b, (slot // 4 + 2 * core) % 4))
            inner_w = jnp.minimum(slot % 3 + inner_b % 2, 3)
            at_w = jnp.where(slot < 12, inner_w, jnp.where(slot < 16, 3 - 3 * (edge_b % 2), slot % 4))
            before = window_half(b, at_w, i // 2)
            whole = (before + got[32 * w : 32 * w + 32]).astype(BF)
            acc[part] = whole.astype(F32)
            normed[part] = layer_norm(whole.astype(F32))
        return 0

    lax.fori_loop(0, 4, proj_one, 0)

    def feed(rows, k):
        up = wf[:, :, :, :, :, k, pl.ds(0, 8)].reshape(D, D)
        hidden = lax.dot_general(normed[rows], up, (((1,), (1,)), ((), ())), preferred_element_type=F32)
        hidden = jax.nn.gelu(hidden).astype(BF)
        down = wf[:, :, :, :, :, k, pl.ds(8, 8)].reshape(D, D)
        acc[rows] += jnp.dot(hidden, down, preferred_element_type=F32)

    def feed_sent(k, _):
        pump_at("big", k, 3)
        feed(pl.ds(384, 640), k)
        return 0

    def feed_kept(k, _):
        feed(pl.ds(0, 384), k)
        return 0

    def finish_other(samples):
        for b in samples:
            mine, other, _, _, _, edge, _ = geometry(b)
            for j in range(5):
                left = acc[pl.ds(pl.multiple_of(other_row(b, max(j - 1, 0)), 32), 32)]
                right = acc[pl.ds(pl.multiple_of(other_row(b, min(j, 3)), 32), 32)]
                back[b, other, j] = jnp.where(early, left, right).astype(BF).reshape(4, 8, D)
        for b in samples:
            returns(b, 0).start()
            returns(b, 2).start()

    lax.fori_loop(0, 3, feed_sent, 0)
    pump("big3")
    feed(pl.ds(768, 256), 3)
    pl.when(core == 1)(lambda: finish_other((0, 1)))
    pl.when(core == 0)(lambda: finish_other((2, 3)))
    feed(pl.ds(384, 384), 3)
    for b in range(4):
        mine, _, _, _, _, edge, _ = geometry(b)
        back[b, mine, edge] = acc[pl.ds(384 + 32 * b, 32)].astype(BF).reshape(4, 8, D)
        returns(b, 1).start()
    pl.when(core == 1)(lambda: finish_other((2, 3)))
    pl.when(core == 0)(lambda: finish_other((0, 1)))

    lax.fori_loop(0, 4, feed_kept, 0)

    def keep(b):
        mine, _, _, _, off, _, _ = geometry(b)
        return pltpu.make_async_copy(back.at[b, mine, pl.ds(off, 4)], out.at[b, mine], o_sem.at[b])

    for b in range(4):
        mine, _, _, _, _, edge, _ = geometry(b)
        for j in range(5):
            if j != edge:
                left = acc[pl.ds(own_row(b, max(j - 1, 0)), 32)]
                right = acc[pl.ds(own_row(b, min(j, 3)), 32)]
                back[b, mine, j] = jnp.where(early, left, right).astype(BF).reshape(4, 8, D)
        keep(b).start()
    for b in range(4):
        keep(b).wait()
        for k in range(3):
            returns(b, k).wait_recv()

    for n in NAMES:
        for m in range(COUNT[n]):
            send(n, m).wait_send()
    for b in range(4):
        for k in range(6):
            halo(b, k).wait_send()
        for k in range(3):
            returns(b, k).wait_send()


def merge_kernel(got, side, out):
    out[...] = got[...]
    late = lax.broadcasted_iota(jnp.int32, (64, D), 0) % 8 >= 4
    from_side = side[...].astype(F32).reshape(64, D)
    odd = pl.program_id(0) % 2 == 1

    @pl.when(jnp.logical_not(odd))
    def _():
        here = got[0, :, 0].astype(F32).reshape(64, D)
        out[0, :, 0] = jnp.where(late, here, from_side).astype(BF).reshape(8, 8, D)

    @pl.when(odd)
    def _():
        here = got[0, :, 3].astype(F32).reshape(64, D)
        out[0, :, 3] = jnp.where(late, from_side, here).astype(BF).reshape(8, 8, D)


def per_device(tokens, qkv_weight, proj_weight, up_weight, down_weight, bias_table, sea_mask):
    hbm = pl.BlockSpec(memory_space=pl.ANY)
    vmem = pl.BlockSpec(memory_space=pltpu.VMEM)
    shard = (2, 4, 2, 2, 4)
    tile = (4, 8, 4, 8, D)
    messages = sum(COUNT.values())
    dma = pltpu.SemaphoreType.DMA
    got, side = pl.pallas_call(
        block_kernel,
        out_shape=(jax.ShapeDtypeStruct(tile, BF), jax.ShapeDtypeStruct((4, 8, 8, D), BF)),
        in_specs=[hbm] * 5 + [vmem, vmem],
        out_specs=(hbm, hbm),
        scratch_shapes=[
            pltpu.VMEM(shard + (24, D), BF),
            pltpu.VMEM(shard + (8, D), BF),
            pltpu.VMEM(shard + (4, 16, D), BF),
            pltpu.VMEM((4, 8, 5, 8, D), BF),
            pltpu.VMEM((1024, D), BF),
            pltpu.VMEM((1024, 3 * D), BF),
            pltpu.VMEM((1024, D), BF),
            pltpu.VMEM((1024, D), F32),
            pltpu.VMEM((4, 8, 5, 8, D), BF),
            pltpu.VMEM((4, 15, 16, 256), F32),
            pltpu.VMEM((4, 64, 256), F32),
            pltpu.VMEM((16, 128), F32),
            dma((messages,)),
            dma((messages,)),
            dma((4,)),
            dma((24,)),
            dma((24,)),
            dma((12,)),
            dma((12,)),
            dma((4,)),
            dma((4,)),
        ],
        compiler_params=pltpu.CompilerParams(
            collective_id=0, has_side_effects=True, vmem_limit_bytes=67043328
        ),
        name="swin_block",
    )(
        tokens.reshape(tile), qkv_weight, proj_weight, up_weight.reshape(4, 8, D), down_weight.reshape(4, 8, D),
        bias_table, sea_mask,
    )
    out = pl.pallas_call(
        merge_kernel,
        grid=(4,),
        out_shape=jax.ShapeDtypeStruct(tile, BF),
        in_specs=[
            pl.BlockSpec((1, 8, 4, 8, D), lambda b: (b, 0, 0, 0, 0)),
            pl.BlockSpec((1, 8, 8, D), lambda b: (b, 0, 0, 0)),
        ],
        out_specs=pl.BlockSpec((1, 8, 4, 8, D), lambda b: (b, 0, 0, 0, 0)),
        name="merge_borders",
    )(got, side)
    return out.reshape(tokens.shape)


def solution(mesh):
    placed = (
        P(None, "lat", "lon", None),
        P(("lat", "lon"), None),
        P(("lat", "lon"), None),
        P(("lat", "lon"), None),
        P(("lat", "lon"), None),
        P(),
        P(),
    )
    return jax.shard_map(
        per_device,
        mesh=mesh,
        in_specs=placed,
        out_specs=P(None, "lat", "lon", None),
        check_vma=False,
    )
```

```python
import jax
import jax.numpy as jnp
from jax import lax
from jax.experimental import pallas as pl
from jax.experimental.pallas import tpu as pltpu
from jax.sharding import PartitionSpec as P

MESH = pl.DeviceIdType.MESH
BF = jnp.bfloat16
F32 = jnp.float32
D = 1024
FAR = -1e30
TOGETHER = 4

PIECES = (
    (0, 0, 0, 1024, "xyz"),
    (0, 8, 0, 1024, "yzx"),
    (0, 16, 0, 1024, "xzy"),
    (1, 0, 0, 1024, "yxz"),
    (2, 0, 0, 512, "zxy"),
    (2, 0, 512, 256, "xyz"),
    (2, 0, 768, 256, "xyz"),
    (2, 1, 0, 256, "yzx"),
    (2, 1, 256, 384, "yzx"),
    (2, 1, 640, 384, "xzy"),
    (2, 2, 0, 512, "zxy"),
    (2, 2, 512, 256, "yxz"),
    (2, 2, 768, 256, "yzx"),
    (2, 3, 0, 512, "yzx"),
    (2, 3, 512, 256, "zyx"),
    (2, 3, 768, 256, "xzy"),
)
NAMES = range(len(PIECES))
FINE = (0, 1, 2)
COUNT = [27 if n in FINE else 15 for n in NAMES]
START = [sum(COUNT[:n]) for n in NAMES]
FINE_STEPS = {
    1: ((), (0, 1, 2)),
    2: ((0, 1, 2), (3, 4, 7, 8)),
    3: ((3, 4), (5, 6, 11, 12, 15, 16)),
    4: ((5, 6), (19, 20, 23)),
    5: ((7, 8), (9, 10)),
    6: ((11, 12, 15, 16), (13, 14, 17, 18)),
    7: ((19, 20), (21, 22, 24, 25)),
    8: ((9, 10, 13, 14, 17, 18, 21, 22), (26,)),
    9: ((23, 24, 25, 26), ()),
}
STEPS = {
    1: ((), (0, 1, 2)),
    2: ((0, 1, 2), (3, 4)),
    3: ((3, 4), (5, 6)),
    4: ((5, 6), (7, 8, 11)),
    5: ((7, 8), (9, 10, 12, 13)),
    6: ((9, 10), (14,)),
    7: ((11, 12, 13, 14), ()),
}
BEGIN, KEYS, BIAS, NORM_OWN, NORM_OTHER, QKV, ATTEND, PROJ, FEED = 0, 1, 2, 3, 4, 10, 20, 40, 50

PLAN = (
    (0, 1, 0), (0, 1, 1), (0, 1, 2), (0, 0, 4), (0, 0, 5), (0, 1, 3), (0, 1, 4), (0, 1, 5), (0, 1, 6), (0, 1, 7),
    (0, 1, 8), (0, 1, 9), (0, 1, 10), (0, 1, 11), (0, 1, 12), (0, 1, 13), (0, 1, 14), (0, 1, 15), (3, 2, 0), (3, 2, 1),
    (3, 2, 4), (3, 2, 2), (3, 0, 0), (3, 0, 2), (3, 0, 3), (3, 2, 10), (3, 2, 14), (3, 2, 3), (3, 2, 7), (3, 2, 8),
    (4, 2, 11), (4, 2, 12), (4, 3, 1), (4, 2, 13), (4, 3, 0), (4, 3, 2), (4, 2, 5), (4, 2, 6), (4, 3, 7), (4, 2, 9),
    (4, 3, 8), (4, 2, 15), (4, 3, 12), (4, 4, 1), (4, 5, 1), (4, 3, 4), (4, 3, 13), (4, 3, 10), (4, 3, 14), (4, 4, 0),
    (4, 5, 0), (4, 3, 3), (4, 6, 0), (4, 3, 11), (4, 4, 2), (4, 0, 1), (4, 5, 2), (4, 6, 2), (4, 3, 9), (4, 3, 5),
    (4, 6, 1), (4, 3, 6), (4, 3, 15), (4, 7, 1), (4, 7, 2), (4, 7, 0), (4, 4, 7), (4, 4, 8), (4, 4, 4), (4, 4, 3),
    (10, 4, 5), (10, 4, 9), (10, 8, 0), (10, 8, 1), (10, 8, 2), (10, 9, 0), (10, 9, 1), (10, 9, 2), (11, 5, 7), (11, 4, 12),
    (12, 5, 3), (12, 5, 4), (12, 4, 6), (12, 4, 10), (13, 5, 8), (13, 4, 13), (20, 5, 5), (20, 6, 7), (20, 4, 11), (21, 5, 9),
    (21, 4, 15), (23, 5, 12), (23, 4, 14), (24, 6, 3), (24, 7, 7), (26, 6, 4), (27, 6, 8), (28, 7, 3), (29, 5, 6), (30, 7, 4),
    (30, 7, 8), (31, 6, 5), (34, 7, 5), (40, 5, 10), (40, 5, 11), (41, 5, 13), (42, 6, 6), (42, 6, 9), (42, 6, 12), (50, 7, 6),
    (50, 7, 9), (50, 7, 12), (50, 5, 14), (50, 5, 15), (50, 6, 11), (51, 6, 10), (51, 7, 11), (51, 6, 13), (52, 7, 10), (52, 7, 13),
    (52, 6, 14), (52, 6, 15), (53, 7, 14), (53, 7, 15),
)


def planned(slot):
    return [(what, name) for where, what, name in PLAN if where == slot]


def block_kernel(
    tok, wq_in, wp_in, wu_in, wd_in, table, sea,
    out, side,
    wq, wp, wf, ext, normed, qkv, att, acc, back, spread, bias, keys,
    w_send, w_recv, own_sem, h_send, h_recv, r_send, r_recv, t_sem, o_sem,
):
    lat = lax.axis_index("lat")
    lon = lax.axis_index("lon")
    core = lat % 2
    y = (lat // 2) % 4
    z_lo = lat // 8
    x = lon % 4
    z_hi = lon // 4
    at = {"x": x, "y": y, "z": z_hi * 2 + z_lo}

    def device(over, partner=False):
        c = dict(at)
        c.update(over)
        k = 1 - core if partner else core
        return {"lat": ((c["z"] % 2) * 4 + c["y"]) * 2 + k, "lon": (c["z"] // 2) * 4 + c["x"]}

    ring = {a: [at[a]] + [(at[a] + by) % 4 for by in (1, 2, 3)] for a in "xyz"}

    def near(axis, by):
        return ring[axis][by % 4]

    def shifted(d_lat, d_lon):
        return {"lat": (lat + d_lat + 16) % 16, "lon": (lon + d_lon + 8) % 8}

    held = (wq, wp, wf)

    def region(name, c, where):
        which, first, col, cols, _ = PIECES[name]
        ref = held[which]

        def part(axis):
            v = where[axis]
            if v is None:
                return slice(None)
            if isinstance(v, tuple):
                return pl.ds(2 * v[1], 2)
            return v

        v = where["z"]
        if v is None:
            lo, hi = slice(None), slice(None)
        elif isinstance(v, tuple):
            lo, hi = v[1], slice(None)
        else:
            lo, hi = v % 2, v // 2
        rows = (first, slice(None)) if which == 2 else (pl.ds(first, 8),)
        return ref.at[(lo, part("y"), c, hi, part("x"), *rows, pl.ds(col, cols))]

    targets = {(a, by): device({a: near(a, by)}) for a in "xyz" for by in (1, 2, 3)}
    partner = device({}, True)

    def message(name, m):
        a1, a2, a3 = PIECES[name][4]
        here = dict(at)
        if m < 3:
            by = (1, 3, 2)[m]
            return here, {**here, a1: near(a1, -by)}, targets[a1, by]
        m -= 3
        line = {**here, a1: None}
        plane = {**line, a2: None}
        if m < 4:
            axis, whole = a2, line
        elif name in FINE and m < 20:
            axis, whole = a3, {**line, a2: near(a2, (0, 3, 1, 2)[(m - 4) // 4])}
        elif m < 8:
            axis, whole = a3, plane
        else:
            by = (0, 1, 3, 2)[m - (20 if name in FINE else 8)]
            sent = {**plane, a3: near(a3, by)}
            return sent, sent, partner
        m %= 4
        if m < 2:
            by = 1 if m == 0 else 3
            return whole, {**whole, axis: near(axis, -by)}, targets[axis, by]
        by = 1 if m == 2 else 3
        half = {**whole, a1: ("h", m - 2)}
        return {**half, axis: near(axis, -by)}, {**half, axis: near(axis, 2)}, targets[axis, by]

    def weight_copy(name, m, where, to):
        k = START[name] + m
        there = region(name, core, where)
        return pltpu.make_async_remote_copy(
            src_ref=there, dst_ref=there, send_sem=w_send.at[k], recv_sem=w_recv.at[k],
            device_id=to, device_id_type=MESH,
        )

    def send(name, m):
        sent, _, to = message(name, m)
        return weight_copy(name, m, sent, to)

    def came(name, m):
        _, landed, to = message(name, m)
        return weight_copy(name, m, landed, to)

    def step(number, name):
        awaited, sent = (FINE_STEPS if name in FINE else STEPS)[number]
        for m in awaited:
            came(name, m).wait_recv()
        for m in sent:
            send(name, m).start()

    def pump(slot):
        for what, name in planned(slot):
            if what == 0:
                for b in (0, 2, 1, 3):
                    halo(b, name).start()
            else:
                step(what, name)

    def pump_at(base, i, count, together=1):
        for k in range(count):
            if planned(base + k):
                @pl.when(i == k // together)
                def _(k=k):
                    pump(base + k)

    def geometry(b):
        ahead = b < 2
        right = b % 2 == 0
        mine = pl.ds(4, 4) if ahead else pl.ds(0, 4)
        other = pl.ds(0, 4) if ahead else pl.ds(4, 4)
        d_lat = 1 if ahead else -1
        d_lon = 1 if right else -1
        off = 0 if right else 1
        edge = 4 if right else 0
        border = 0 if right else 3
        return mine, other, d_lat, d_lon, off, edge, border

    def halo(b, k):
        _, other, d_lat, d_lon, off, edge, border = geometry(b)
        mine_first, other_first = (4, 0) if b < 2 else (0, 4)
        mine = pl.ds(mine_first, 4)
        if k < 4:
            src, dst = tok.at[b, other_first + k], ext.at[b, other_first + k, pl.ds(off, 4)]
            to = shifted(-d_lat, 0)
        elif k == 4:
            src, dst, to = tok.at[b, mine, border], ext.at[b, mine, edge], shifted(0, -d_lon)
        else:
            src, dst, to = tok.at[b, other, border], ext.at[b, other, edge], shifted(-d_lat, -d_lon)
        return pltpu.make_async_remote_copy(
            src_ref=src, dst_ref=dst, send_sem=h_send.at[6 * b + k], recv_sem=h_recv.at[6 * b + k],
            device_id=to, device_id_type=MESH,
        )

    def local_tokens(b):
        mine, _, _, _, off, _, _ = geometry(b)
        return pltpu.make_async_copy(tok.at[b, mine], ext.at[b, mine, pl.ds(off, 4)], t_sem.at[b])

    def returns(b, k):
        mine, other, d_lat, d_lon, off, edge, _ = geometry(b)
        src, dst, to = (
            (back.at[b, other, pl.ds(off, 4)], out.at[b, other], (d_lat, 0)),
            (back.at[b, mine, edge], side.at[b, mine], (0, d_lon)),
            (back.at[b, other, edge], side.at[b, other], (d_lat, d_lon)),
        )[k]
        return pltpu.make_async_remote_copy(
            src_ref=src, dst_ref=dst, send_sem=r_send.at[3 * b + k], recv_sem=r_recv.at[3 * b + k],
            device_id=shifted(*to), device_id_type=MESH,
        )

    def own(which):
        here = (z_lo, y, core, z_hi, x)
        src, dst = (
            (wq_in, wq.at[here]),
            (wp_in, wp.at[here]),
            (wu_in, wf.at[(*here, slice(None), pl.ds(0, 8))]),
            (wd_in, wf.at[(*here, slice(None), pl.ds(8, 8))]),
        )[which]
        return pltpu.make_async_copy(src, dst, own_sem.at[which])

    for which in range(4):
        own(which).start()
    for b in range(4):
        local_tokens(b).start()

    barrier = pltpu.get_barrier_semaphore()
    peers = list(targets.values()) + [partner]
    peers += [shifted(i, j) for i in (-1, 0, 1) for j in (-1, 0, 1) if (i, j) != (0, 0)]
    for peer in peers:
        pl.semaphore_signal(barrier, inc=1, device_id=peer, device_id_type=MESH)
    pl.semaphore_wait(barrier, len(peers))

    for which in range(4):
        own(which).wait()
    pump(BEGIN)

    pump(KEYS)
    spot = lax.broadcasted_iota(jnp.int32, (256, 512), 1)
    spot_col = spot % 8
    spot_window = spot // 128
    grid_col = lax.broadcasted_iota(jnp.int32, (256, 512), 0)
    own_row = lax.broadcasted_iota(jnp.int32, (8, 512), 0) == (lax.broadcasted_iota(jnp.int32, (8, 512), 1) // 8) % 8
    for b in range(4):
        row = lat if b < 2 else (lat + 15) % 16
        block = lon * 4 + (0 if b % 2 == 0 else 31)
        upper = sea[pl.ds(pl.multiple_of(row * 8, 8), 8)]
        lower = sea[pl.ds(pl.multiple_of(((row + 1) % 16) * 8, 8), 8)]
        band = jnp.concatenate([upper[4:], lower[:4]], axis=0)
        open_at = jnp.where(band == 1, 1.0, 0.0).astype(BF)
        wanted = ((block + spot_window + jnp.where(spot_col < 4, 1, 0)) * 8 + spot_col) % 256
        chosen = jnp.where(grid_col == wanted, 1.0, 0.0).astype(BF)
        found = jnp.dot(open_at, chosen, preferred_element_type=F32)
        found = jnp.sum(jnp.where(own_row, found, 0.0), axis=0, keepdims=True)
        closed = jnp.where(found > 0.5, 0.0, FAR)
        for w in range(4):
            keys[4 * b + w : 4 * b + w + 1] = closed[:, 128 * w : 128 * w + 128]

    pump(BIAS)
    lane = lax.broadcasted_iota(jnp.int32, (16, 256), 1)
    head_row = lax.broadcasted_iota(jnp.int32, (16, 256), 0)
    lane_row = (lane % 64) // 8
    col_step = (lax.broadcasted_iota(jnp.int32, (8, 256), 0) + 4) % 8 - (
        lax.broadcasted_iota(jnp.int32, (8, 256), 1) + 4
    ) % 8 + 7
    for g in range(4):
        over_lanes = jnp.where(head_row == 4 * g + lane // 64, 1.0, 0.0)
        wide = jnp.dot(
            table[...], over_lanes, precision=lax.Precision.HIGHEST, preferred_element_type=F32
        )
        for d in range(15):
            spread[g, d, 0:15] = wide[15 * d : 15 * d + 15]

    def bias_one(i, _):
        g, r = i // 8, i % 8
        steps = jnp.zeros((16, 256), F32)
        for k in range(8):
            steps = jnp.where(lane_row == k, spread[g, r - k + 7], steps)
        line = jnp.zeros((8, 256), F32)
        for d in range(15):
            line = jnp.where(col_step == d, steps[d : d + 1], line)
        bias[g, pl.ds(pl.multiple_of(r * 8, 8), 8)] = line
        return 0

    lax.fori_loop(0, 32, bias_one, 0)

    def other_row(b, w):
        return 512 + 128 * ((b + 2 * core) % 4) + 32 * w

    def own_row(b, w):
        if isinstance(b, int):
            edge_here = w == (3 if b % 2 == 0 else 0)
            return 384 + 32 * b if edge_here else 32 * (3 * b + w - b % 2)
        odd = b % 2
        edge_here = w == 3 - 3 * odd
        return jnp.where(edge_here, 384 + 32 * b, 32 * (3 * b + w - odd))

    early = lax.broadcasted_iota(jnp.int32, (32, D), 0) % 8 < 4

    def window_half(b, w, half):
        rows = pl.ds(jnp.where((b < 2) == (half == 0), 4, 0), 4)
        left = ext[b, rows, w].astype(F32).reshape(32, D)
        right = ext[b, rows, w + 1].astype(F32).reshape(32, D)
        return jnp.where(early, right, left)

    def layer_norm(v):
        centre = jnp.mean(v, axis=-1, keepdims=True)
        moved = v - centre
        spread_of = jnp.mean(moved * moved, axis=-1, keepdims=True)
        return (moved * lax.rsqrt(spread_of + 1e-05)).astype(BF)

    def norm_half(half):
        def norm_one(i, _):
            first = (other_row if half else own_row)(i // 4, i % 4)
            rows = pl.ds(pl.multiple_of(first, 32), 32)
            normed[rows] = layer_norm(window_half(i // 4, i % 4, half))
            return 0

        lax.fori_loop(0, 16, norm_one, 0)

    pump(NORM_OWN)
    for b in range(4):
        local_tokens(b).wait()
        halo(b, 4).wait_recv()
    norm_half(0)
    pump(NORM_OTHER)
    for b in range(4):
        for k in (0, 1, 2, 3, 5):
            halo(b, k).wait_recv()
    norm_half(1)

    def qkv_one(i, _):
        pump_at(QKV, i, 4)
        w = wq[i // 2, pl.ds((i % 2) * 2, 2)].reshape(768, D)
        got = lax.dot_general(normed[...], w, (((1,), (1,)), ((), ())), preferred_element_type=F32)
        qkv[:, pl.ds(pl.multiple_of(i * 768, 768), 768)] = got.astype(BF)
        return 0

    lax.fori_loop(0, 4, qkv_one, 0)

    lane_head = lax.broadcasted_iota(jnp.int32, (64, 256), 1) // 64
    pick = [lane_head == h for h in range(4)]
    ones_at = (
        lax.broadcasted_iota(jnp.int32, (256, 256), 0) // 64
        == lax.broadcasted_iota(jnp.int32, (256, 256), 1) // 64
    )
    ones = jnp.where(ones_at, 1.0, 0.0).astype(BF)
    first_half = lax.broadcasted_iota(jnp.int32, (64, 128), 1) < 64
    q_cell = lax.broadcasted_iota(jnp.int32, (64, 128), 0)
    k_cell = lax.broadcasted_iota(jnp.int32, (64, 128), 1) % 64
    itself = q_cell == k_cell
    parted = (q_cell < 32) != (k_cell < 32)

    def spread_heads(v):
        wide = v.astype(F32)
        return jnp.concatenate([jnp.where(p, wide, 0.0).astype(BF) for p in pick], axis=0)

    def attend_one(i):
        owned, foreign = own_row(i // 4, i % 4), other_row(i // 4, i % 4)
        top = pl.ds(pl.multiple_of(jnp.where(i < 8, owned, foreign), 32), 32)
        low = pl.ds(pl.multiple_of(jnp.where(i < 8, foreign, owned), 32), 32)

        def cut(first):
            return jnp.concatenate([qkv[top, pl.ds(first, 256)], qkv[low, pl.ds(first, 256)]], axis=0)

        at_end = jnp.where(i < 8, lat, (lat + 15) % 16) == 15
        end_value = jnp.where(at_end, FAR, 0.0)
        mask = jnp.where(itself, 0.0, jnp.broadcast_to(keys[pl.ds(i, 1)], (64, 128)))
        mask = jnp.where(parted, mask + end_value, mask)
        for g in range(4):
            q, k, v = cut(256 * g), cut(D + 256 * g), cut(2 * D + 256 * g)
            scores = lax.dot_general(
                q, spread_heads(k), (((1,), (1,)), ((), ())), preferred_element_type=F32
            )
            weights = []
            for t in range(2):
                s = scores[:, 128 * t : 128 * t + 128] * 0.125 + bias[g, :, pl.ds(128 * t, 128)] + mask
                top_a = jnp.max(jnp.where(first_half, s, -jnp.inf), axis=1, keepdims=True)
                top_b = jnp.max(jnp.where(first_half, -jnp.inf, s), axis=1, keepdims=True)
                weights.append(jnp.exp(s - jnp.where(first_half, top_a, top_b)).astype(BF))
            e = jnp.concatenate(weights, axis=1)
            total = jnp.dot(e, ones, preferred_element_type=F32)
            context = jnp.dot(e, spread_heads(v), preferred_element_type=F32) / total
            att[top, pl.ds(256 * g, 256)] = context[:32].astype(BF)
            att[low, pl.ds(256 * g, 256)] = context[32:].astype(BF)

    def attend_some(i, _):
        pump_at(ATTEND, i, 16, TOGETHER)
        for u in range(TOGETHER):
            attend_one(i * TOGETHER + u)
        return 0

    lax.fori_loop(0, 16 // TOGETHER, attend_some, 0)

    def proj_one(i, _):
        pump_at(PROJ, i, 4, 2)
        rows = pl.ds(pl.multiple_of(i * 512, 512), 512)
        got = lax.dot_general(
            att[rows], wp[...].reshape(D, D), (((1,), (1,)), ((), ())), preferred_element_type=F32
        )
        for w in range(16):
            part = pl.ds(pl.multiple_of(i * 512 + w * 32, 32), 32)
            slot = i * 16 + w
            edge_b = jnp.clip(slot - 12, 0, 3)
            inner_b = jnp.minimum(slot // 3, 3)
            b = jnp.where(slot < 12, inner_b, jnp.where(slot < 16, edge_b, (slot // 4 + 2 * core) % 4))
            inner_w = jnp.minimum(slot % 3 + inner_b % 2, 3)
            at_w = jnp.where(slot < 12, inner_w, jnp.where(slot < 16, 3 - 3 * (edge_b % 2), slot % 4))
            before = window_half(b, at_w, i)
            whole = (before + got[32 * w : 32 * w + 32]).astype(BF)
            acc[part] = whole.astype(F32)
            normed[part] = layer_norm(whole.astype(F32))
        return 0

    lax.fori_loop(0, 2, proj_one, 0)

    def feed(rows, k):
        up = wf[:, :, :, :, :, k, pl.ds(0, 8)].reshape(D, D)
        hidden = lax.dot_general(normed[rows], up, (((1,), (1,)), ((), ())), preferred_element_type=F32)
        hidden = jax.nn.gelu(hidden).astype(BF)
        down = wf[:, :, :, :, :, k, pl.ds(8, 8)].reshape(D, D)
        acc[rows] += jnp.dot(hidden, down, preferred_element_type=F32)

    def feed_sent(k, _):
        pump_at(FEED, k, 3)
        feed(pl.ds(384, 640), k)
        return 0

    def feed_kept(k, _):
        feed(pl.ds(0, 384), k)
        return 0

    def finish_other(samples):
        for b in samples:
            mine, other, _, _, _, edge, _ = geometry(b)
            for j in range(5):
                left = acc[pl.ds(pl.multiple_of(other_row(b, max(j - 1, 0)), 32), 32)]
                right = acc[pl.ds(pl.multiple_of(other_row(b, min(j, 3)), 32), 32)]
                back[b, other, j] = jnp.where(early, left, right).astype(BF).reshape(4, 8, D)
        for b in samples:
            returns(b, 0).start()
            returns(b, 2).start()

    lax.fori_loop(0, 3, feed_sent, 0)
    pump(FEED + 3)
    feed(pl.ds(768, 256), 3)
    pl.when(core == 1)(lambda: finish_other((0, 1)))
    pl.when(core == 0)(lambda: finish_other((2, 3)))
    feed(pl.ds(384, 384), 3)
    for b in range(4):
        mine, _, _, _, _, edge, _ = geometry(b)
        back[b, mine, edge] = acc[pl.ds(384 + 32 * b, 32)].astype(BF).reshape(4, 8, D)
        returns(b, 1).start()
    pl.when(core == 1)(lambda: finish_other((2, 3)))
    pl.when(core == 0)(lambda: finish_other((0, 1)))

    lax.fori_loop(0, 4, feed_kept, 0)

    def keep(b):
        mine, _, _, _, off, _, _ = geometry(b)
        return pltpu.make_async_copy(back.at[b, mine, pl.ds(off, 4)], out.at[b, mine], o_sem.at[b])

    for b in range(4):
        mine, _, _, _, _, edge, _ = geometry(b)
        for j in range(5):
            if j != edge:
                left = acc[pl.ds(own_row(b, max(j - 1, 0)), 32)]
                right = acc[pl.ds(own_row(b, min(j, 3)), 32)]
                back[b, mine, j] = jnp.where(early, left, right).astype(BF).reshape(4, 8, D)
        keep(b).start()
    for b in range(4):
        keep(b).wait()
        for k in range(3):
            returns(b, k).wait_recv()

    for n in NAMES:
        for m in range(COUNT[n]):
            send(n, m).wait_send()
    for b in range(4):
        for k in range(6):
            halo(b, k).wait_send()
        for k in range(3):
            returns(b, k).wait_send()


def merge_kernel(got, side, out, held, halves, in_sem, side_sem, out_sem):
    late = lax.broadcasted_iota(jnp.int32, (64, D), 0) % 8 >= 4

    def moves(b):
        return (
            pltpu.make_async_copy(side.at[b], halves.at[b], side_sem.at[b]),
            pltpu.make_async_copy(got.at[b], held.at[b], in_sem.at[b]),
            pltpu.make_async_copy(held.at[b], out.at[b], out_sem.at[b]),
        )

    for b in range(4):
        moves(b)[0].start()
        moves(b)[1].start()
    for b in range(4):
        moves(b)[0].wait()
        moves(b)[1].wait()
        border = 0 if b % 2 == 0 else 3
        here = held[b, :, border].astype(F32).reshape(64, D)
        there = halves[b].astype(F32).reshape(64, D)
        both = jnp.where(late, here, there) if b % 2 == 0 else jnp.where(late, there, here)
        held[b, :, border] = both.astype(BF).reshape(8, 8, D)
        moves(b)[2].start()
    for b in range(4):
        moves(b)[2].wait()


def per_device(tokens, qkv_weight, proj_weight, up_weight, down_weight, bias_table, sea_mask):
    hbm = pl.BlockSpec(memory_space=pl.ANY)
    vmem = pl.BlockSpec(memory_space=pltpu.VMEM)
    shard = (2, 4, 2, 2, 4)
    tile = (4, 8, 4, 8, D)
    messages = sum(COUNT)
    dma = pltpu.SemaphoreType.DMA
    got, side = pl.pallas_call(
        block_kernel,
        out_shape=(jax.ShapeDtypeStruct(tile, BF), jax.ShapeDtypeStruct((4, 8, 8, D), BF)),
        in_specs=[hbm] * 5 + [vmem, vmem],
        out_specs=(hbm, hbm),
        scratch_shapes=[
            pltpu.VMEM(shard + (24, D), BF),
            pltpu.VMEM(shard + (8, D), BF),
            pltpu.VMEM(shard + (4, 16, D), BF),
            pltpu.VMEM((4, 8, 5, 8, D), BF),
            pltpu.VMEM((1024, D), BF),
            pltpu.VMEM((1024, 3 * D), BF),
            pltpu.VMEM((1024, D), BF),
            pltpu.VMEM((1024, D), F32),
            pltpu.VMEM((4, 8, 5, 8, D), BF),
            pltpu.VMEM((4, 15, 16, 256), F32),
            pltpu.VMEM((4, 64, 256), F32),
            pltpu.VMEM((16, 128), F32),
            dma((messages,)),
            dma((messages,)),
            dma((4,)),
            dma((24,)),
            dma((24,)),
            dma((12,)),
            dma((12,)),
            dma((4,)),
            dma((4,)),
        ],
        compiler_params=pltpu.CompilerParams(
            collective_id=0, has_side_effects=True, vmem_limit_bytes=67043328
        ),
        name="swin_block",
    )(
        tokens.reshape(tile), qkv_weight, proj_weight, up_weight.reshape(4, 8, D), down_weight.reshape(4, 8, D),
        bias_table, sea_mask,
    )
    out = pl.pallas_call(
        merge_kernel,
        out_shape=jax.ShapeDtypeStruct(tile, BF),
        in_specs=[hbm, hbm],
        out_specs=hbm,
        scratch_shapes=[
            pltpu.VMEM(tile, BF),
            pltpu.VMEM((4, 8, 8, D), BF),
            dma((4,)),
            dma((4,)),
            dma((4,)),
        ],
        name="merge_borders",
    )(got, side)
    return out.reshape(tokens.shape)


def solution(mesh):
    placed = (
        P(None, "lat", "lon", None),
        P(("lat", "lon"), None),
        P(("lat", "lon"), None),
        P(("lat", "lon"), None),
        P(("lat", "lon"), None),
        P(),
        P(),
    )
    return jax.shard_map(
        per_device,
        mesh=mesh,
        in_specs=placed,
        out_specs=P(None, "lat", "lon", None),
        check_vma=False,
    )
```
